256 devices in a mesh: dp: 32 (over x, z), col: 8 (over y, core).
Axes of the slice: x: 4, y: 4, z: 8, core: 2. Of those that a mesh axis runs over, the one named last changes fastest.
Arguments:
- activations: bfloat16 [2, 28672, 8192], P(None, 'dp', 'col'), may hold values from -40 to 40
- cotangent: bfloat16 [2, 28672, 2048], P(None, 'dp'), may hold values from -40 to 40
- master_weights: float32 [2, 2048, 8192], P(None, 'dp', 'col'), may hold values from -6 to 6
- moment_codes: bfloat16 [2, 2048, 8192], P(None, 'dp', 'col'), may hold values from -1 to 1
- square_codes: bfloat16 [2, 2048, 8192], P(None, 'dp', 'col'), may hold values from 0.049804688 to 1
- moment_scales: float32 [2, 2048, 4], P(None, 'dp'), may hold values from 0.05 to 0.5
- square_scales: float32 [2, 2048, 4], P(None, 'dp'), may hold values from 0.005 to 0.05
Outputs:
- new_weights: float32 [2, 2048, 8192], P(None, 'dp', 'col')
- new_moment_codes: bfloat16 [2, 2048, 8192], P(None, 'dp', 'col')
- new_square_codes: bfloat16 [2, 2048, 8192], P(None, 'dp', 'col')
- new_moment_scales: float32 [2, 2048, 4], P(None, 'dp')
- new_square_scales: float32 [2, 2048, 4], P(None, 'dp')
The draws below stay inside these ranges and needn't reach their ends.
All inputs are finite; a program needn't handle non-finite values. Where the reference program divides by a largest or mean magnitude, that divisor is 1e-20 or more.
Results may differ from the reference program's by a relative error of at most 0.001.
Values sent between devices are 32-bit elements; how exact they have to be, the bound alone decides.
A program may use at most 128 MiB of HBM per device.

```python
import math
import jax
import jax.numpy as jnp
from jax import lax

D = 8192
KV = 2048
BLOCK = 2048
LAYERS = 2
STEP = 10
TOK_DEV = 896
TOKENS = 28672
NB = 4
N_DP = 32


def scaled_values(key, width):
    keys = jax.random.split(key, 2)
    position = jnp.arange(width, dtype=jnp.float32) / width
    col_scale = jnp.exp(jnp.log(3.0) * position + jnp.log(3.4) * jax.random.uniform(keys[1], (width,)))
    values = jax.random.normal(keys[0], (LAYERS, TOKENS, width)) * col_scale
    return jnp.clip(values, -40.0, 40.0).astype(jnp.bfloat16)


def draw_activations(key, part):
    return scaled_values(jax.random.fold_in(key, 11), D)


def draw_cotangent(key, part):
    return scaled_values(jax.random.fold_in(key, 23), KV)


def shard_levels(stream_key, shape, cuts, smallest, high):
    def one(axis_at, parts):
        heights = jax.random.uniform(jax.random.fold_in(jax.random.fold_in(stream_key, 6), axis_at), (parts,), jnp.float32, smallest / len(cuts), high / len(cuts))
        return jnp.repeat(jnp.exp(heights), shape[axis_at] // parts).reshape((-1,) + (1,) * (len(shape) - axis_at - 1))

    gain = one(*cuts[0])
    for cut in cuts[1:]:
        gain = gain * one(*cut)
    return gain


def normal_values(stream_key, shape, scale, limit, shards=(), kind=jnp.bfloat16):
    array = scale * jax.random.normal(stream_key, shape, jnp.float32)
    if shards:
        array = array * shard_levels(stream_key, shape, shards, -0.22, 0.18)
    return jnp.clip(array, -limit, limit).astype(kind)


def setup_inputs(seed: int = 0) -> dict:
    arg_keys = jax.random.split(jax.random.key(seed), 8)
    return {
        "activations": draw_activations(jax.random.fold_in(arg_keys[7], 71), 0),
        "cotangent": draw_cotangent(jax.random.fold_in(arg_keys[7], 71), 0),
        "master_weights": normal_values(arg_keys[2], (LAYERS, KV, D), 1.0, 6.0, ((1, 32), (2, 8)), jnp.float32),
        "moment_codes": jnp.clip(jax.random.uniform(arg_keys[3], (LAYERS, KV, D), jnp.float32, -1.0, 1.0) * shard_levels(arg_keys[3], (LAYERS, KV, D), ((1, 32), (2, 8)), -0.4, 0.0), -1.0, 1.0).astype(jnp.bfloat16),
        "square_codes": jnp.clip(0.049804688 + 0.9501953 * jax.random.uniform(arg_keys[4], (LAYERS, KV, D), jnp.float32) ** shard_levels(arg_keys[4], (LAYERS, KV, D), ((1, 32), (2, 8)), -0.2, 0.2), 0.049804688, 1.0).astype(jnp.bfloat16),
        "moment_scales": jnp.clip(jnp.exp(math.log(0.5) - 2.3025851 * jax.random.uniform(arg_keys[5], (LAYERS, KV, NB), jnp.float32) ** shard_levels(arg_keys[5], (LAYERS, KV, NB), ((1, 32),), -0.2, 0.2)), 0.05, 0.5),
        "square_scales": jnp.clip(jnp.exp(math.log(0.05) - 2.3025851 * jax.random.uniform(arg_keys[6], (LAYERS, KV, NB), jnp.float32) ** shard_levels(arg_keys[6], (LAYERS, KV, NB), ((1, 32),), -0.2, 0.2)), 0.005, 0.05),
    }


beta_one = 0.9
beta_two = 0.999
learn_rate = 0.001
decay_rate = 0.1
adam_eps = 1e-08
scale_eps = 1e-06
norm_eps = 1e-06

def layer_gradient(layer_acts, layer_cot):
    grouped_acts = layer_acts.reshape(N_DP, TOK_DEV, D)
    grouped_cot = layer_cot.reshape(N_DP, TOK_DEV, KV)

    def accumulate(total, pair):
        group_acts, group_cot = pair
        partial_sum = lax.dot_general(group_cot, group_acts, (((0,), (0,)), ((), ())), preferred_element_type=jnp.float32)
        return (total + partial_sum, None)
    total, unused = lax.scan(accumulate, jnp.zeros((KV, D), jnp.float32), (grouped_acts, grouped_cot))
    return total

def reference(activations, cotangent, master_weights, moment_codes, square_codes, moment_scales, square_scales):
    gradients = [layer_gradient(activations[index], cotangent[index]) for index in range(LAYERS)]
    total_sq = jnp.float32(0.0)
    for gradient in gradients:
        total_sq = total_sq + jnp.sum(gradient * gradient)
    rms = jnp.sqrt(total_sq / float(LAYERS * KV * D) + norm_eps)
    clip_factor = jnp.minimum(1.0, 1.0 / rms)
    correct_one = 1.0 - beta_one ** STEP
    correct_two = 1.0 - beta_two ** STEP
    outs_weights, outs_mcode, outs_scode, outs_mscale, outs_sscale = ([], [], [], [], [])
    for index in range(LAYERS):
        old_moment = moment_codes[index].astype(jnp.float32).reshape(KV, NB, BLOCK) * moment_scales[index][:, :, None]
        old_square = square_codes[index].astype(jnp.float32).reshape(KV, NB, BLOCK) * square_scales[index][:, :, None]
        grad_now = (clip_factor * gradients[index]).reshape(KV, NB, BLOCK)
        moment = beta_one * old_moment + (1.0 - beta_one) * grad_now
        square = beta_two * old_square + (1.0 - beta_two) * grad_now * grad_now
        moment_max = lax.optimization_barrier(jnp.max(jnp.abs(moment), axis=2))
        square_max = lax.optimization_barrier(jnp.max(square, axis=2))
        outs_mcode.append((moment / (moment_max[:, :, None] + scale_eps)).astype(jnp.bfloat16).reshape(KV, D))
        outs_scode.append((square / (square_max[:, :, None] + scale_eps)).astype(jnp.bfloat16).reshape(KV, D))
        outs_mscale.append(moment_max)
        outs_sscale.append(square_max)
        ratio = (moment / correct_one / (jnp.sqrt(square / correct_two) + adam_eps)).reshape(KV, D)
        weights = master_weights[index]
        outs_weights.append(weights - learn_rate * (decay_rate * weights + ratio))
    return (jnp.stack(outs_weights), jnp.stack(outs_mcode), jnp.stack(outs_scode), jnp.stack(outs_mscale), jnp.stack(outs_sscale))
```

```python
import functools
import heapq

import jax
import jax.numpy as jnp
from jax import lax
from jax.experimental import pallas as pl
from jax.experimental.pallas import tpu as pltpu
from jax.sharding import Mesh
from jax.sharding import PartitionSpec as P

D = 8192
KV = 2048
BLOCK = 2048
LAYERS = 2
STEP = 10

beta_one = 0.9
beta_two = 0.999
learn_rate = 0.001
decay_rate = 0.1
adam_eps = 1e-08
scale_eps = 1e-06
norm_eps = 1e-06

NX, NZ, NY, NC = 4, 8, 4, 2
ROWS = KV // (NX * NZ)
COLS = D // (NY * NC)
TOK = 896
XROWS = ROWS * NZ
CA = 640
CB = COLS - CA
WINDOW_A, WINDOW_B = 3, 2
NT = 512
MESH = pl.DeviceIdType.MESH
F32 = jnp.float32


def task_order(rate=46.6e3, latency=2.3, add=0.1, matmul=2.0):
    bytes_a, bytes_b = ROWS * CA * 4, ROWS * CB * 4
    now, order, free, heap, seen = 0.0, [], {}, [], set()
    matmuls = [("M", d, s, 0) for s in range(NX) for d in (0, 1)]
    arrived, count, serial = [], 0, 0
    total = 2 * (NZ * (NX - 1) + NZ - 1 + NX * (NZ - 1) + NX - 1)

    def ready(task):
        kind, d, j, s = task
        need = {
            "A": ("M", d, s + 1, 0),
            "B": ("M", d, j, 0),
            "ZA": ("A", d, s + 1, NX - 2),
            "XB": ("B", d, j + 1, NZ - 2),
        }[kind]
        return need in seen

    def enabled(task):
        kind, d, j, s = task
        out = []
        if kind == "M":
            if j == 0:
                out += [("A", d, q, 0) for q in range(WINDOW_A)]
            if j < WINDOW_B:
                out.append(("B", d, j, 0))
        elif kind == "A":
            if s < NX - 2:
                out.append(("A", d, j, s + 1))
            else:
                if j == 0:
                    out.append(("ZA", d, 0, 0))
                if j + WINDOW_A < NZ:
                    out.append(("A", d, j + WINDOW_A, 0))
        elif kind == "B":
            if s < NZ - 2:
                out.append(("B", d, j, s + 1))
            else:
                if j == 0:
                    out.append(("XB", d, 0, 0))
                if j + WINDOW_B < NX:
                    out.append(("B", d, j + WINDOW_B, 0))
        elif kind == "ZA":
            if s < NZ - 2:
                out.append(("ZA", d, 0, s + 1))
        elif kind == "XB":
            if j < NX - 2:
                out.append(("XB", d, j + 1, 0))
        return out

    while count < total or matmuls:
        while heap and heap[0][0] <= now:
            arrived.append(heapq.heappop(heap))
        able = [a for a in arrived if ready(a[2])]
        if able:
            first = min(able)
            arrived.remove(first)
            task = first[2]
            now += add
            count += 1
        elif matmuls:
            task = matmuls.pop(0)
            now += matmul
        else:
            now = max(now, heap[0][0])
            continue
        seen.add(task)
        sends = enabled(task)
        for send in sends:
            link = ("x" if send[0] in ("A", "XB") else "z", send[1])
            size = bytes_a if send[0] in ("A", "ZA") else bytes_b
            free[link] = max(now, free.get(link, 0.0)) + size / rate
            heapq.heappush(heap, (free[link] + latency, serial, send))
            serial += 1
        order.append((task, sends))
    return order


def kernel(
    act_hbm, cot_hbm, master_hbm, mcode_hbm, scode_hbm, mscale_hbm, sscale_hbm,
    weights_out, mcode_out, scode_out, mscale_out, sscale_out,
    act, cot, master, mcode, scode, mscale, sscale,
    part, buf_a, buf_za, buf_b, buf_xb, grad, mom, sqr, norm_send, norm_recv, top_send, top_recv, gather,
    in_sems, send_a, recv_a, send_za, recv_za, send_b, recv_b, send_xb, recv_xb,
    norm_send_sems, norm_recv_sems, top_sems, gather_send_sems, gather_recv_sems,
):
    x, z, y, c = (lax.axis_index(n) for n in ("x", "z", "y", "core"))
    sign = (1, -1)

    def wrap(v, n):
        return lax.rem(v + 2 * n, n)

    def xrel(d, s):
        return wrap(x - sign[d] * (1 + s), NX)

    def zrel(d, s):
        return wrap(z - sign[d] * (1 + s), NZ)

    loads = {}

    def load(name, src, dst, k):
        loads[name] = pltpu.make_async_copy(src, dst, in_sems.at[k])
        loads[name].start()

    def cot_columns(d, s):
        return pl.ds(pl.multiple_of(xrel(d, s) * XROWS, XROWS), XROWS)

    k = 0
    for s in range(NX):
        for d in (0, 1):
            if s == 0:
                load(("act", d), act_hbm.at[d], act.at[d], k)
                k += 1
            load(("cot", d, s), cot_hbm.at[d, :, cot_columns(d, s)], cot.at[d, s], k)
            k += 1
    for name, src, dst in (
        ("master", master_hbm, master), ("mcode", mcode_hbm, mcode), ("scode", scode_hbm, scode),
        ("mscale", mscale_hbm, mscale), ("sscale", sscale_hbm, sscale),
    ):
        load(name, src, dst, k)
        k += 1

    col_peers = [(dy, dc) for dy in range(NY) for dc in range(NC) if dy or dc]
    barrier = pltpu.get_barrier_semaphore()
    peers = (
        [{"x": wrap(x + i, NX)} for i in range(1, NX)]
        + [{"z": wrap(z + i, NZ)} for i in range(1, NZ)]
        + [{"y": wrap(y + dy, NY), "core": wrap(c + dc, NC)} for dy, dc in col_peers]
    )
    for peer in peers:
        pl.semaphore_signal(barrier, inc=1, device_id=peer, device_id_type=MESH)

    def rows_z(d, j):
        return pl.ds(pl.multiple_of(zrel(d, j) * ROWS, ROWS), ROWS)

    def own_a(d, j, s):
        return part.at[d, s, rows_z(d, j), pl.ds(0, CA)]

    def own_b(d, j, s):
        return part.at[d, j, rows_z(d, s), pl.ds(CA, CB)]

    def copy_of(task):
        kind, d, j, s = task
        if kind == "A":
            i = j * (NX - 1) + s
            src = own_a(d, j, 0) if s == 0 else buf_a.at[d, i - 1]
            dst, ssem, rsem, axis = buf_a.at[d, i], send_a.at[d, i], recv_a.at[d, i], "x"
        elif kind == "ZA":
            src = buf_a.at[d, NX - 2] if s == 0 else buf_za.at[d, s - 1]
            dst, ssem, rsem, axis = buf_za.at[d, s], send_za.at[d, s], recv_za.at[d, s], "z"
        elif kind == "B":
            i = j * (NZ - 1) + s
            src = own_b(d, j, 0) if s == 0 else buf_b.at[d, i - 1]
            dst, ssem, rsem, axis = buf_b.at[d, i], send_b.at[d, i], recv_b.at[d, i], "z"
        else:
            src = buf_b.at[d, NZ - 2] if j == 0 else buf_xb.at[d, j - 1]
            dst, ssem, rsem, axis = buf_xb.at[d, j], send_xb.at[d, j], recv_xb.at[d, j], "x"
        target = wrap(x + sign[d], NX) if axis == "x" else wrap(z + sign[d], NZ)
        return pltpu.make_async_remote_copy(
            src_ref=src, dst_ref=dst, send_sem=ssem, recv_sem=rsem,
            device_id={axis: target}, device_id_type=MESH,
        )

    def add_own(task):
        kind, d, j, s = task
        if kind == "A":
            i = j * (NX - 1) + s
            buf_a[d, i] = buf_a[d, i] + own_a(d, j, s + 1)[...]
        elif kind == "ZA":
            mine = buf_a[d, (s + 1) * (NX - 1) + NX - 2]
            if s == NZ - 2:
                grad[d, :, :CA] = buf_za[d, s] + mine
            else:
                buf_za[d, s] = buf_za[d, s] + mine
        elif kind == "B":
            i = j * (NZ - 1) + s
            buf_b[d, i] = buf_b[d, i] + own_b(d, j, s + 1)[...]
        else:
            mine = buf_b[d, (j + 1) * (NZ - 1) + NZ - 2]
            if j == NX - 2:
                grad[d, :, CA:] = buf_xb[d, j] + mine
            else:
                buf_xb[d, j] = buf_xb[d, j] + mine

    def matmul(d, s):
        if s == 0:
            loads[("act", d)].wait()
        loads[("cot", d, s)].wait()

        @pl.loop(0, COLS // NT)
        def _(n):
            cols = pl.ds(pl.multiple_of(n * NT, NT), NT)
            part[d, s, :, cols] = lax.dot_general(
                cot[d, s], act[d, :, cols], (((0,), (0,)), ((), ())), preferred_element_type=F32
            )

    started = []
    first = True
    for task, sends in task_order():
        if task[0] == "M":
            matmul(task[1], task[2])
            if first:
                pl.semaphore_wait(barrier, len(peers))
                first = False
        else:
            copy_of(task).wait_recv()
            add_own(task)
        for send in sends:
            copy = copy_of(send)
            copy.start()
            started.append(copy)

    total = jnp.zeros((8, 128), F32)
    for d in range(LAYERS):
        for r in range(ROWS // 8):
            v = grad[d, pl.ds(r * 8, 8), :]
            v = v * v
            for i in range(COLS // 128):
                total = total + v[:, i * 128 : (i + 1) * 128]
    line = jnp.sum(total, axis=0, keepdims=True)
    stages = (
        [({"y": wrap(y + dy, NY), "core": wrap(c + dc, NC)}) for dy, dc in col_peers],
        [{"x": wrap(x + i, NX)} for i in range(1, NX)],
        [{"z": wrap(z + i, NZ)} for i in range(1, NZ)],
    )
    base = 0
    for n, stage in enumerate(stages):
        norm_send[n] = line
        copies = []
        for i, peer in enumerate(stage):
            copy = pltpu.make_async_remote_copy(
                src_ref=norm_send.at[n], dst_ref=norm_recv.at[base + i],
                send_sem=norm_send_sems.at[base + i], recv_sem=norm_recv_sems.at[base + i],
                device_id=peer, device_id_type=MESH,
            )
            copy.start()
            copies.append(copy)
        for i, copy in enumerate(copies):
            copy.wait_recv()
            line = line + norm_recv[base + i]
        started += copies
        base += len(stage)
    total_sq = jnp.sum(line, axis=1, keepdims=True)
    rms = jnp.sqrt(total_sq / float(LAYERS * KV * D) + norm_eps)
    clip = jnp.minimum(1.0, 1.0 / rms)

    for name in ("master", "mcode", "scode", "mscale", "sscale"):
        loads[name].wait()
    diagonal = lax.broadcasted_iota(jnp.int32, (ROWS, 128), 0) == lax.broadcasted_iota(
        jnp.int32, (ROWS, 128), 1
    )
    diagonal_in = diagonal[:, :ROWS]

    def to_row(column):
        return jnp.sum(jnp.where(diagonal, column, 0.0), axis=0, keepdims=True)

    def to_column(row):
        return jnp.sum(jnp.where(diagonal_in, row, 0.0), axis=1, keepdims=True)

    def own_block(scales, d):
        mine = lax.broadcasted_iota(jnp.int32, (NY, ROWS), 0) == y
        return to_column(jnp.sum(jnp.where(mine, scales[d], 0.0), axis=0, keepdims=True))

    rows = []
    for d in range(LAYERS):
        moment_scale = own_block(mscale, d)
        square_scale = own_block(sscale, d)
        old_moment = mcode[d].astype(F32) * moment_scale
        old_square = scode[d].astype(F32) * square_scale
        grad_now = clip * grad[d]
        moment = beta_one * old_moment + (1.0 - beta_one) * grad_now
        square = beta_two * old_square + (1.0 - beta_two) * grad_now * grad_now
        mom[d] = moment
        sqr[d] = square
        rows.append(to_row(jnp.max(jnp.abs(moment), axis=1, keepdims=True)))
        rows.append(to_row(jnp.max(square, axis=1, keepdims=True)))
    top = jnp.concatenate(rows + [jnp.zeros((4, 128), F32)], axis=0)

    top_send[...] = top
    copy = pltpu.make_async_remote_copy(
        src_ref=top_send, dst_ref=top_recv, send_sem=top_sems.at[0], recv_sem=top_sems.at[1],
        device_id={"core": 1 - c}, device_id_type=MESH,
    )
    copy.start()
    started.append(copy)
    copy.wait_recv()
    top = jnp.maximum(top, top_recv[...])
    gather[y] = top
    copies = []
    for i in range(1, NY):
        copy = pltpu.make_async_remote_copy(
            src_ref=gather.at[y], dst_ref=gather.at[y],
            send_sem=gather_send_sems.at[i - 1], recv_sem=gather_recv_sems.at[i - 1],
            device_id={"y": wrap(y + i, NY)}, device_id_type=MESH,
        )
        copy.start()
        started.append(copy)
        incoming = gather.at[wrap(y - i, NY)]
        copies.append(pltpu.make_async_remote_copy(
            src_ref=incoming, dst_ref=incoming,
            send_sem=gather_send_sems.at[i - 1], recv_sem=gather_recv_sems.at[i - 1],
            device_id={"y": wrap(y + i, NY)}, device_id_type=MESH,
        ))

    correct_one = 1.0 - beta_one**STEP
    correct_two = 1.0 - beta_two**STEP
    for d in range(LAYERS):
        moment_div = to_column(top[2 * d : 2 * d + 1, :ROWS]) + scale_eps
        square_div = to_column(top[2 * d + 1 : 2 * d + 2, :ROWS]) + scale_eps
        moment = mom[d]
        square = sqr[d]
        mcode_out[d] = (moment / moment_div).astype(jnp.bfloat16)
        scode_out[d] = (square / square_div).astype(jnp.bfloat16)
        ratio = moment / correct_one / (jnp.sqrt(square / correct_two) + adam_eps)
        weights = master[d]
        weights_out[d] = weights - learn_rate * (decay_rate * weights + ratio)

    for copy in copies:
        copy.wait_recv()
    for b in range(NY):
        for d in range(LAYERS):
            mscale_out[d, b : b + 1, :] = gather[b, 2 * d : 2 * d + 1, :ROWS]
            sscale_out[d, b : b + 1, :] = gather[b, 2 * d + 1 : 2 * d + 2, :ROWS]
    for copy in started:
        copy.wait_send()


def local(
    activations, cotangent, master_weights, moment_codes, square_codes, moment_scales, square_scales
):
    shard = (LAYERS, ROWS, COLS)
    scales = (LAYERS, NY, ROWS)
    any_spec = pl.BlockSpec(memory_space=pl.ANY)
    vmem_spec = pl.BlockSpec(memory_space=pltpu.VMEM)
    sems = pltpu.SemaphoreType.DMA
    n_norm = (NY * NC - 1) + (NX - 1) + (NZ - 1)
    outs = pl.pallas_call(
        kernel,
        out_shape=(
            jax.ShapeDtypeStruct(shard, F32),
            jax.ShapeDtypeStruct(shard, jnp.bfloat16),
            jax.ShapeDtypeStruct(shard, jnp.bfloat16),
            jax.ShapeDtypeStruct(scales, F32),
            jax.ShapeDtypeStruct(scales, F32),
        ),
        in_specs=[any_spec] * 7,
        out_specs=[vmem_spec] * 5,
        scratch_shapes=[
            pltpu.VMEM((LAYERS, TOK, COLS), jnp.bfloat16),
            pltpu.VMEM((LAYERS, NX, TOK, XROWS), jnp.bfloat16),
            pltpu.VMEM(shard, F32),
            pltpu.VMEM(shard, jnp.bfloat16),
            pltpu.VMEM(shard, jnp.bfloat16),
            pltpu.VMEM(scales, F32),
            pltpu.VMEM(scales, F32),
            pltpu.VMEM((LAYERS, NX, XROWS, COLS), F32),
            pltpu.VMEM((2, NZ * (NX - 1), ROWS, CA), F32),
            pltpu.VMEM((2, NZ - 1, ROWS, CA), F32),
            pltpu.VMEM((2, NX * (NZ - 1), ROWS, CB), F32),
            pltpu.VMEM((2, NX - 1, ROWS, CB), F32),
            pltpu.VMEM(shard, F32),
            pltpu.VMEM(shard, F32),
            pltpu.VMEM(shard, F32),
            pltpu.VMEM((3, 1, 128), F32),
            pltpu.VMEM((n_norm, 1, 128), F32),
            pltpu.VMEM((8, 128), F32),
            pltpu.VMEM((8, 128), F32),
            pltpu.VMEM((NY, 8, 128), F32),
            sems((2 * (NX + 1) + 5,)),
            sems((2, NZ * (NX - 1))), sems((2, NZ * (NX - 1))),
            sems((2, NZ - 1)), sems((2, NZ - 1)),
            sems((2, NX * (NZ - 1))), sems((2, NX * (NZ - 1))),
            sems((2, NX - 1)), sems((2, NX - 1)),
            sems((n_norm,)), sems((n_norm,)), sems((2,)), sems((NY - 1,)), sems((NY - 1,)),
        ],
        compiler_params=pltpu.CompilerParams(
            collective_id=0, has_side_effects=True, vmem_limit_bytes=60 * 1024 * 1024
        ),
    )(
        activations, cotangent, master_weights, moment_codes, square_codes,
        jnp.transpose(moment_scales, (0, 2, 1)), jnp.transpose(square_scales, (0, 2, 1)),
    )
    return (*outs[:3], jnp.transpose(outs[3], (0, 2, 1)), jnp.transpose(outs[4], (0, 2, 1)))


def solution(mesh):
    split = Mesh(mesh.devices.reshape(NX, NZ, NY, NC), ("x", "z", "y", "core"))
    dp, col = ("x", "z"), ("y", "core")
    big, scale = P(None, dp, col), P(None, dp, None)
    return jax.shard_map(
        local,
        mesh=split,
        in_specs=(big, scale, big, big, big, scale, scale),
        out_specs=(big, big, big, scale, scale),
        check_vma=False,
    )
```

```python
import functools
import heapq

import jax
import jax.numpy as jnp
from jax import lax
from jax.experimental import pallas as pl
from jax.experimental.pallas import tpu as pltpu
from jax.sharding import Mesh
from jax.sharding import PartitionSpec as P

D = 8192
KV = 2048
BLOCK = 2048
LAYERS = 2
STEP = 10

beta_one = 0.9
beta_two = 0.999
learn_rate = 0.001
decay_rate = 0.1
adam_eps = 1e-08
scale_eps = 1e-06
norm_eps = 1e-06

NX, NZ, NY, NC = 4, 8, 4, 2
ROWS = KV // (NX * NZ)
COLS = D // (NY * NC)
TOK = 896
XROWS = ROWS * NZ
TILES = COLS // 128
BLOCK_ROWS = TILES * ROWS
RA = 304
RB = BLOCK_ROWS - RA
WINDOW_A, WINDOW_B = 2, 4
MESH = pl.DeviceIdType.MESH
F32 = jnp.float32


def task_order(rate=44e3, latency=2.5, add=0.2, matmul=2.0):
    bytes_a, bytes_b = RA * 512, RB * 512
    now, order, free, heap, seen = 0.0, [], {}, [], set()
    matmuls = [("M", d, s, h) for s in range(NX) for d in (0, 1) for h in ((1, 0) if s == 0 else (2,))]
    arrived, count, serial = [], 0, 0
    total = 2 * (NZ * (NX - 1) + NZ - 1 + NX * (NZ - 1) + NX - 1)

    def ready(task):
        kind, d, j, s = task
        need = {
            "A": ("M", d, s + 1, 2),
            "B": ("M", d, j, 2 if j else 1),
            "ZA": ("A", d, s + 1, NX - 2),
            "XB": ("B", d, j + 1, NZ - 2),
        }[kind]
        return need in seen

    def enabled(task):
        kind, d, j, s = task
        out = []
        if kind == "M":
            if j == 0 and s == 0:
                out += [("A", d, q, 0) for q in range(WINDOW_A)]
            if j < WINDOW_B and s:
                out.append(("B", d, j, 0))
        elif kind == "A":
            if s < NX - 2:
                out.append(("A", d, j, s + 1))
            else:
                if j == 0:
                    out.append(("ZA", d, 0, 0))
                if j + WINDOW_A < NZ:
                    out.append(("A", d, j + WINDOW_A, 0))
        elif kind == "B":
            if s < NZ - 2:
                out.append(("B", d, j, s + 1))
            else:
                if j == 0:
                    out.append(("XB", d, 0, 0))
                if j + WINDOW_B < NX:
                    out.append(("B", d, j + WINDOW_B, 0))
        elif kind == "ZA":
            if s < NZ - 2:
                out.append(("ZA", d, 0, s + 1))
        elif kind == "XB":
            if j < NX - 2:
                out.append(("XB", d, j + 1, 0))
        return out

    while count < total or matmuls:
        while heap and heap[0][0] <= now:
            arrived.append(heapq.heappop(heap))
        able = [a for a in arrived if ready(a[2])]
        if able:
            first = min(able)
            arrived.remove(first)
            task = first[2]
            now += add
            count += 1
        elif matmuls:
            task = matmuls.pop(0)
            now += matmul if task[3] == 2 else matmul / 2
        else:
            now = max(now, heap[0][0])
            continue
        seen.add(task)
        sends = enabled(task)
        for send in sends:
            link = ("x" if send[0] in ("A", "XB") else "z", send[1])
            size = bytes_a if send[0] in ("A", "ZA") else bytes_b
            free[link] = max(now, free.get(link, 0.0)) + size / rate
            heapq.heappush(heap, (free[link] + latency, serial, send))
            serial += 1
        order.append((task, sends))
    return order


def kernel(
    act_hbm, cot_hbm, mcode_hbm, scode_hbm, mscale_hbm, sscale_hbm,
    grad_out, small_out,
    act, cot, cot_t, mcode, scode, mscale, sscale,
    part, buf_a, buf_za, buf_b, buf_xb, grad, old_m, old_s, norm_send, norm_recv, own_top, tops,
    in_sems, send_sems, recv_sems, recv_a, recv_za, recv_b, recv_xb, out_sems,
):
    x, z, y, c = (lax.axis_index(n) for n in ("x", "z", "y", "core"))
    sign = (1, -1)

    def wrap(v, n):
        return lax.rem(v + 2 * n, n)

    def xrel(d, s):
        return wrap(x - sign[d] * (1 + s), NX)

    def zrel(d, s):
        return wrap(z - sign[d] * (1 + s), NZ)

    loads = {}

    def load(name, src, dst, k):
        loads[name] = pltpu.make_async_copy(src, dst, in_sems.at[k])
        loads[name].start()

    def cot_columns(d, s):
        return pl.ds(pl.multiple_of(xrel(d, s) * XROWS, XROWS), XROWS)

    half = COLS // 2
    groups = []
    for s in range(NX):
        for d in (0, 1):
            group = [(("cot", d, s), cot_hbm.at[d, :, cot_columns(d, s)], cot.at[d, s])]
            if s == 0:
                for h in (1, 0):
                    group.append((("act", d, h), act_hbm.at[d, :, pl.ds(h * half, half)], act.at[d, h]))
            groups.append(group)
    groups.append([
        ("mcode", mcode_hbm, mcode), ("scode", scode_hbm, scode),
        ("mscale", mscale_hbm, mscale), ("sscale", sscale_hbm, sscale),
    ])

    def load_next():
        if groups:
            for name, src, dst in groups.pop(0):
                load(name, src, dst, len(loads))

    load_next()
    col_steps = [(i, j) for i in range(NY) for j in range(NC) if i or j]
    barrier = pltpu.get_barrier_semaphore()
    col_peers = [{"y": wrap(y + i, NY), "core": wrap(c + j, NC)} for i, j in col_steps]
    plane_peers = [
        {"x": wrap(x + i, NX), "z": wrap(z + j, NZ)} for i in range(NX) for j in range(NZ) if i or j
    ]
    stages = (col_peers, plane_peers)
    peers = [{"x": wrap(x + i, NX)} for i in sign] + [{"z": wrap(z + i, NZ)} for i in sign] + col_peers
    for peer in peers:
        pl.semaphore_signal(barrier, inc=1, device_id=peer, device_id_type=MESH)

    def own_a(d, j, s):
        return part.at[d, s, zrel(d, j), pl.ds(0, RA)]

    def own_b(d, j, s):
        return part.at[d, j, zrel(d, s), pl.ds(RA, RB)]

    def copy_of(task):
        kind, d, j, s = task
        if kind == "A":
            i = j * (NX - 1) + s
            src = own_a(d, j, 0) if s == 0 else buf_a.at[d, i - 1]
            dst, ssem, rsem, axis = buf_a.at[d, i], send_sems.at[0], recv_a.at[d, j % 4, s], "x"
        elif kind == "ZA":
            src = buf_a.at[d, NX - 2] if s == 0 else buf_za.at[d, s - 1]
            dst, ssem, rsem, axis = buf_za.at[d, s], send_sems.at[1], recv_za.at[d, s], "z"
        elif kind == "B":
            i = j * (NZ - 1) + s
            src = own_b(d, j, 0) if s == 0 else buf_b.at[d, i - 1]
            dst, ssem, rsem, axis = buf_b.at[d, i], send_sems.at[2], recv_b.at[d, i], "z"
        else:
            src = buf_b.at[d, NZ - 2] if j == 0 else buf_xb.at[d, j - 1]
            dst, ssem, rsem, axis = buf_xb.at[d, j], send_sems.at[3], recv_xb.at[d, j], "x"
        target = wrap(x + sign[d], NX) if axis == "x" else wrap(z + sign[d], NZ)
        return pltpu.make_async_remote_copy(
            src_ref=src, dst_ref=dst, send_sem=ssem, recv_sem=rsem,
            device_id={axis: target}, device_id_type=MESH,
        )

    def add_own(task):
        kind, d, j, s = task
        if kind == "A":
            i = j * (NX - 1) + s
            buf_a[d, i] = buf_a[d, i] + own_a(d, j, s + 1)[...]
        elif kind == "ZA":
            mine = buf_a[d, (s + 1) * (NX - 1) + NX - 2]
            if s == NZ - 2:
                grad[d, :RA] = buf_za[d, s] + mine
            else:
                buf_za[d, s] = buf_za[d, s] + mine
        elif kind == "B":
            i = j * (NZ - 1) + s
            buf_b[d, i] = buf_b[d, i] + own_b(d, j, s + 1)[...]
        else:
            mine = buf_b[d, (j + 1) * (NZ - 1) + NZ - 2]
            if j == NX - 2:
                grad[d, RA:] = buf_xb[d, j] + mine
            else:
                buf_xb[d, j] = buf_xb[d, j] + mine

    def product(d, s, h, start):
        out = jnp.dot(cot_t[...], act[d, h], preferred_element_type=F32)
        for t in range(TILES // 2):
            rows = pl.ds(start + t * ROWS, ROWS)
            for q in range(NZ):
                part[d, s, q, rows] = out[q * ROWS : (q + 1) * ROWS, t * 128 : (t + 1) * 128]

    half_rows = BLOCK_ROWS // 2

    def matmul(d, s, h):
        if s == 0:
            loads[("act", d, h)].wait()
        if h:
            loads[("cot", d, s)].wait()
            cot_t[...] = jnp.transpose(cot[d, s])
        if h != 1:
            load_next()
        if h == 2:

            @pl.loop(0, 2)
            def _(n):
                product(d, s, n, pl.multiple_of(n * half_rows, half_rows))
        else:
            product(d, s, h, h * half_rows)

    def old_state():
        for name in ("mcode", "scode", "mscale", "sscale"):
            loads[name].wait()
        for d in range(LAYERS):
            moment_scale = own_block(mscale[d], y)
            square_scale = own_block(sscale[d], y)
            for t in range(TILES):
                rows, cols = pl.ds(t * ROWS, ROWS), pl.ds(t * 128, 128)
                old_m[d, rows] = beta_one * (mcode[d, :, cols].astype(F32) * moment_scale)
                old_s[d, rows] = beta_two * (scode[d, :, cols].astype(F32) * square_scale)

    first = True
    for task, sends in task_order():
        if task[0] == "M":
            matmul(task[1], task[2], task[3])
            if first:
                pl.semaphore_wait(barrier, len(peers))
                first = False
        else:
            copy_of(task).wait_recv()
            add_own(task)
        for send in sends:
            copy_of(send).start()
        if task == ("M", 1, NX - 1, 2):
            old_state()

    grad_copies = [pltpu.make_async_copy(grad.at[d], grad_out.at[d], out_sems.at[d]) for d in range(LAYERS)]
    for copy in grad_copies:
        copy.start()

    lanes = [jnp.zeros((8, 128), F32) for _ in range(8)]
    for d in range(LAYERS):
        for i in range(BLOCK_ROWS // 8):
            v = grad[d, i * 8 : (i + 1) * 8, :]
            lanes[i % 8] = lanes[i % 8] + v * v
    while len(lanes) > 1:
        lanes = [p + q for p, q in zip(lanes[::2], lanes[1::2])]
    line = jnp.sum(lanes[0], axis=0, keepdims=True)
    def all_of(ref, k):
        return pltpu.make_async_remote_copy(
            src_ref=ref, dst_ref=ref, send_sem=send_sems.at[k], recv_sem=recv_sems.at[max(k - 4, 0)],
            device_id={"core": 1 - c}, device_id_type=MESH,
        )

    base = 0
    for n, stage in enumerate(stages):
        norm_send[n] = line
        for i, peer in enumerate(stage):
            pltpu.make_async_remote_copy(
                src_ref=norm_send.at[n], dst_ref=norm_recv.at[base + i],
                send_sem=send_sems.at[4 + n], recv_sem=recv_sems.at[n],
                device_id=peer, device_id_type=MESH,
            ).start()
        if n == 0:
            for k, buf in enumerate((buf_a, buf_za, buf_b, buf_xb)):
                all_of(buf, k).wait_send()
        incoming = all_of(norm_recv.at[pl.ds(base, len(stage))], 4 + n)
        incoming.wait_recv()
        sums = [norm_recv[base + i] for i in range(len(stage))]
        while len(sums) > 1:
            sums = [sum(sums[i : i + 2]) for i in range(0, len(sums), 2)]
        line = line + sums[0]
        base += len(stage)
    total_sq = jnp.sum(line, axis=1, keepdims=True)
    rms = jnp.sqrt(total_sq / float(LAYERS * KV * D) + norm_eps)
    clip = jnp.minimum(1.0, 1.0 / rms)

    rows = []
    for d in range(LAYERS):
        top_moment = jnp.zeros((ROWS, 128), F32)
        top_square = jnp.zeros((ROWS, 128), F32)
        for t in range(TILES):
            moment, square = moments(
                clip, grad[d, t * ROWS : (t + 1) * ROWS, :],
                old_m[d, t * ROWS : (t + 1) * ROWS, :], old_s[d, t * ROWS : (t + 1) * ROWS, :],
            )
            top_moment = jnp.maximum(top_moment, jnp.abs(moment))
            top_square = jnp.maximum(top_square, square)
        rows.append(to_row(jnp.max(top_moment, axis=1, keepdims=True)))
        rows.append(to_row(jnp.max(top_square, axis=1, keepdims=True)))
    top = jnp.concatenate(rows + [jnp.zeros((4, 128), F32)], axis=0)

    own_top[...] = top
    for i, ((dy, dc), peer) in enumerate(zip(col_steps, col_peers)):
        pltpu.make_async_remote_copy(
            src_ref=own_top, dst_ref=tops.at[i], send_sem=send_sems.at[6], recv_sem=recv_sems.at[2],
            device_id=peer, device_id_type=MESH,
        ).start()
    for n, stage in enumerate(stages):
        all_of(norm_recv.at[pl.ds(0, len(stage))], 4 + n).wait_send()
    for copy in grad_copies:
        copy.wait()
    incoming = all_of(tops, 6)
    incoming.wait_recv()
    same_chip = [i for i, (dy, dc) in enumerate(col_steps) if dy == 0]
    small_out[y] = jnp.maximum(top, tops[same_chip[0]])
    for dy in range(1, NY):
        pair = [tops[i] for i, step in enumerate(col_steps) if step[0] == dy]
        small_out[wrap(y - dy, NY)] = jnp.maximum(*pair)
    small_out[NY] = jnp.broadcast_to(clip, (8, 128))
    incoming.wait_send()


def to_row(column):
    diagonal = lax.broadcasted_iota(jnp.int32, (ROWS, 128), 0) == lax.broadcasted_iota(
        jnp.int32, (ROWS, 128), 1
    )
    return jnp.sum(jnp.where(diagonal, column, 0.0), axis=0, keepdims=True)


def to_column(row):
    diagonal = lax.broadcasted_iota(jnp.int32, (ROWS, ROWS), 0) == lax.broadcasted_iota(
        jnp.int32, (ROWS, ROWS), 1
    )
    return jnp.sum(jnp.where(diagonal, row, 0.0), axis=1, keepdims=True)


def own_block(scales, block):
    mine = lax.broadcasted_iota(jnp.int32, (NY, ROWS), 0) == block
    return to_column(jnp.sum(jnp.where(mine, scales, 0.0), axis=0, keepdims=True))


def moments(clip, grad, old_moment, old_square):
    grad_now = clip * grad
    moment = old_moment + (1.0 - beta_one) * grad_now
    square = old_square + (1.0 - beta_two) * grad_now * grad_now
    return moment, square


def update_kernel(
    grad, small, master, mcode, scode, mscale, sscale,
    weights_out, mcode_out, scode_out, mscale_out, sscale_out,
):
    y = lax.axis_index("y")
    clip = small[NY, :1, :1]
    top = small[y]
    correct_one = 1.0 - beta_one**STEP
    correct_two = 1.0 - beta_two**STEP
    for d in range(LAYERS):
        moment_scale = own_block(mscale[d], y)
        square_scale = own_block(sscale[d], y)
        moment_div = to_column(top[2 * d : 2 * d + 1, :ROWS]) + scale_eps
        square_div = to_column(top[2 * d + 1 : 2 * d + 2, :ROWS]) + scale_eps
        for t in range(TILES):
            cols = pl.ds(t * 128, 128)
            moment, square = moments(
                clip, grad[d, t * ROWS : (t + 1) * ROWS, :],
                beta_one * (mcode[d, :, cols].astype(F32) * moment_scale),
                beta_two * (scode[d, :, cols].astype(F32) * square_scale),
            )
            mcode_out[d, :, cols] = (moment / moment_div).astype(jnp.bfloat16)
            scode_out[d, :, cols] = (square / square_div).astype(jnp.bfloat16)
            ratio = moment / correct_one / (jnp.sqrt(square / correct_two) + adam_eps)
            weights = master[d, :, cols]
            weights_out[d, :, cols] = weights - learn_rate * (decay_rate * weights + ratio)
        for b in range(NY):
            mscale_out[d, b : b + 1, :] = small[b, 2 * d : 2 * d + 1, :ROWS]
            sscale_out[d, b : b + 1, :] = small[b, 2 * d + 1 : 2 * d + 2, :ROWS]


def local(
    activations, cotangent, master_weights, moment_codes, square_codes, moment_scales, square_scales
):
    shard = (LAYERS, ROWS, COLS)
    scales = (LAYERS, NY, ROWS)
    any_spec = pl.BlockSpec(memory_space=pl.ANY)
    vmem_spec = pl.BlockSpec(memory_space=pltpu.VMEM)
    sems = pltpu.SemaphoreType.DMA
    n_norm = NX * NZ - 1 + NY * NC - 1
    block = (LAYERS, BLOCK_ROWS, 128)
    scales_in = (jnp.transpose(moment_scales, (0, 2, 1)), jnp.transpose(square_scales, (0, 2, 1)))
    grad, small = pl.pallas_call(
        kernel,
        out_shape=(
            jax.ShapeDtypeStruct(block, F32),
            jax.ShapeDtypeStruct((NY + 1, 8, 128), F32),
        ),
        in_specs=[any_spec] * 6,
        out_specs=[any_spec, vmem_spec],
        scratch_shapes=[
            pltpu.VMEM((LAYERS, 2, TOK, COLS // 2), jnp.bfloat16),
            pltpu.VMEM((LAYERS, NX, TOK, XROWS), jnp.bfloat16),
            pltpu.VMEM((XROWS, TOK), jnp.bfloat16),
            pltpu.VMEM(shard, jnp.bfloat16),
            pltpu.VMEM(shard, jnp.bfloat16),
            pltpu.VMEM(scales, F32),
            pltpu.VMEM(scales, F32),
            pltpu.VMEM((LAYERS, NX, NZ, BLOCK_ROWS, 128), F32),
            pltpu.VMEM((2, NZ * (NX - 1), RA, 128), F32),
            pltpu.VMEM((2, NZ - 1, RA, 128), F32),
            pltpu.VMEM((2, NX * (NZ - 1), RB, 128), F32),
            pltpu.VMEM((2, NX - 1, RB, 128), F32),
            pltpu.VMEM(block, F32),
            pltpu.VMEM(block, F32),
            pltpu.VMEM(block, F32),
            pltpu.VMEM((2, 1, 128), F32),
            pltpu.VMEM((n_norm, 1, 128), F32),
            pltpu.VMEM((8, 128), F32),
            pltpu.VMEM((NY * NC - 1, 8, 128), F32),
            sems((2 * (NX + 2) + 4,)), sems((7,)), sems((3,)),
            sems((2, 4, NX - 1)), sems((2, NZ - 1)), sems((2, NX * (NZ - 1))), sems((2, NX - 1)),
            sems((LAYERS,)),
        ],
        compiler_params=pltpu.CompilerParams(
            collective_id=0, has_side_effects=True, vmem_limit_bytes=58 * 1024 * 1024
        ),
    )(activations, cotangent, moment_codes, square_codes, *scales_in)
    outs = pl.pallas_call(
        update_kernel,
        out_shape=(
            jax.ShapeDtypeStruct(shard, F32),
            jax.ShapeDtypeStruct(shard, jnp.bfloat16),
            jax.ShapeDtypeStruct(shard, jnp.bfloat16),
            jax.ShapeDtypeStruct(scales, F32),
            jax.ShapeDtypeStruct(scales, F32),
        ),
        in_specs=[vmem_spec] * 7,
        out_specs=[vmem_spec] * 5,
    )(grad, small, master_weights, moment_codes, square_codes, *scales_in)
    return (*outs[:3], jnp.transpose(outs[3], (0, 2, 1)), jnp.transpose(outs[4], (0, 2, 1)))


def solution(mesh):
    split = Mesh(mesh.devices.reshape(NX, NZ, NY, NC), ("x", "z", "y", "core"))
    dp, col = ("x", "z"), ("y", "core")
    big, scale = P(None, dp, col), P(None, dp, None)
    return jax.shard_map(
        local,
        mesh=split,
        in_specs=(big, scale, big, big, big, scale, scale),
        out_specs=(big, big, big, scale, scale),
        check_vma=False,
    )
```

```python
import functools
import heapq

import jax
import jax.numpy as jnp
from jax import lax
from jax.experimental import pallas as pl
from jax.experimental.pallas import tpu as pltpu
from jax.sharding import Mesh
from jax.sharding import PartitionSpec as P

D = 8192
KV = 2048
BLOCK = 2048
LAYERS = 2
STEP = 10

beta_one = 0.9
beta_two = 0.999
learn_rate = 0.001
decay_rate = 0.1
adam_eps = 1e-08
scale_eps = 1e-06
norm_eps = 1e-06

NX, NZ, NY, NC = 4, 8, 4, 2
ROWS = KV // (NX * NZ)
COLS = D // (NY * NC)
TOK = 896
XROWS = ROWS * NZ
TILES = COLS // 128
BLOCK_ROWS = TILES * ROWS
RA = 304
RB = BLOCK_ROWS - RA
WINDOW_A, WINDOW_B = 2, 4
MESH = pl.DeviceIdType.MESH
F32 = jnp.float32


def task_order(rate=44e3, latency=2.5, add=0.2, matmul=2.0):
    bytes_a, bytes_b = RA * 512, RB * 512
    now, order, free, heap, seen = 0.0, [], {}, [], set()
    matmuls = [("M", d, s, h) for s in range(NX) for d in (0, 1) for h in ((1, 0) if s == 0 else (2,))]
    arrived, count, serial = [], 0, 0
    total = 2 * (NZ * (NX - 1) + NZ - 1 + NX * (NZ - 1) + NX - 1)

    def ready(task):
        kind, d, j, s = task
        need = {
            "A": ("M", d, s + 1, 2),
            "B": ("M", d, j, 2 if j else 1),
            "ZA": ("A", d, s + 1, NX - 2),
            "XB": ("B", d, j + 1, NZ - 2),
        }[kind]
        return need in seen

    def enabled(task):
        kind, d, j, s = task
        out = []
        if kind == "M":
            if j == 0 and s == 0:
                out += [("A", d, q, 0) for q in range(WINDOW_A)]
            if j < WINDOW_B and s:
                out.append(("B", d, j, 0))
        elif kind == "A":
            if s < NX - 2:
                out.append(("A", d, j, s + 1))
            else:
                if j == 0:
                    out.append(("ZA", d, 0, 0))
                if j + WINDOW_A < NZ:
                    out.append(("A", d, j + WINDOW_A, 0))
        elif kind == "B":
            if s < NZ - 2:
                out.append(("B", d, j, s + 1))
            else:
                if j == 0:
                    out.append(("XB", d, 0, 0))
                if j + WINDOW_B < NX:
                    out.append(("B", d, j + WINDOW_B, 0))
        elif kind == "ZA":
            if s < NZ - 2:
                out.append(("ZA", d, 0, s + 1))
        elif kind == "XB":
            if j < NX - 2:
                out.append(("XB", d, j + 1, 0))
        return out

    while count < total or matmuls:
        while heap and heap[0][0] <= now:
            arrived.append(heapq.heappop(heap))
        able = [a for a in arrived if ready(a[2])]
        if able:
            first = min(able)
            arrived.remove(first)
            task = first[2]
            now += add
            count += 1
        elif matmuls:
            task = matmuls.pop(0)
            now += matmul if task[3] == 2 else matmul / 2
        else:
            now = max(now, heap[0][0])
            continue
        seen.add(task)
        sends = enabled(task)
        for send in sends:
            link = ("x" if send[0] in ("A", "XB") else "z", send[1])
            size = bytes_a if send[0] in ("A", "ZA") else bytes_b
            free[link] = max(now, free.get(link, 0.0)) + size / rate
            heapq.heappush(heap, (free[link] + latency, serial, send))
            serial += 1
        order.append((task, sends))
    return order


def kernel(
    act_hbm, cot_hbm, mcode_hbm, scode_hbm, mscale_hbm, sscale_hbm,
    grad_out, small_hbm,
    act, cot, cot_t, mcode, scode, mscale, sscale,
    part, buf_a, buf_za, buf_b, buf_xb, grad, old_m, old_s, norm_send, norm_recv, own_top, tops, small_out,
    in_sems, send_sems, recv_sems, recv_a, recv_za, recv_b, recv_xb, out_sems,
):
    x, z, y, c = (lax.axis_index(n) for n in ("x", "z", "y", "core"))
    sign = (1, -1)

    def wrap(v, n):
        return lax.rem(v + 2 * n, n)

    def xrel(d, s):
        return wrap(x - sign[d] * (1 + s), NX)

    def zrel(d, s):
        return wrap(z - sign[d] * (1 + s), NZ)

    loads = {}

    def load(name, src, dst, k):
        loads[name] = pltpu.make_async_copy(src, dst, in_sems.at[k])
        loads[name].start()

    def cot_columns(d, s):
        return pl.ds(pl.multiple_of(xrel(d, s) * XROWS, XROWS), XROWS)

    half = COLS // 2
    groups = []
    for s in range(NX):
        for d in (0, 1):
            group = [(("cot", d, s), cot_hbm.at[d, :, cot_columns(d, s)], cot.at[d, s])]
            if s == 0:
                for h in (1, 0):
                    group.append((("act", d, h), act_hbm.at[d, :, pl.ds(h * half, half)], act.at[d, h]))
            groups.append(group)
    groups.append([
        ("mcode", mcode_hbm, mcode), ("scode", scode_hbm, scode),
        ("mscale", mscale_hbm, mscale), ("sscale", sscale_hbm, sscale),
    ])

    def load_next():
        if groups:
            for name, src, dst in groups.pop(0):
                load(name, src, dst, len(loads))

    load_next()
    col_steps = [(i, j) for i in range(NY) for j in range(NC) if i or j]
    barrier = pltpu.get_barrier_semaphore()
    col_peers = [{"y": wrap(y + i, NY), "core": wrap(c + j, NC)} for i, j in col_steps]
    stages = (
        [{"x": wrap(x + i, NX), "y": wrap(y + j, NY)} for i in range(NX) for j in range(NY) if i or j],
        [{"z": wrap(z + i, NZ), "core": wrap(c + j, NC)} for i in range(NZ) for j in range(NC) if i or j],
    )
    peers = [{"x": wrap(x + i, NX)} for i in sign] + [{"z": wrap(z + i, NZ)} for i in sign] + col_peers
    for peer in peers:
        pl.semaphore_signal(barrier, inc=1, device_id=peer, device_id_type=MESH)

    def own_a(d, j, s):
        return part.at[d, s, zrel(d, j), pl.ds(0, RA)]

    def own_b(d, j, s):
        return part.at[d, j, zrel(d, s), pl.ds(RA, RB)]

    def copy_of(task):
        kind, d, j, s = task
        if kind == "A":
            i = j * (NX - 1) + s
            src = own_a(d, j, 0) if s == 0 else buf_a.at[d, i - 1]
            dst, ssem, rsem, axis = buf_a.at[d, i], send_sems.at[0], recv_a.at[d, j % 4, s], "x"
        elif kind == "ZA":
            src = buf_a.at[d, NX - 2] if s == 0 else buf_za.at[d, s - 1]
            dst, ssem, rsem, axis = buf_za.at[d, s], send_sems.at[1], recv_za.at[d, s], "z"
        elif kind == "B":
            i = j * (NZ - 1) + s
            src = own_b(d, j, 0) if s == 0 else buf_b.at[d, i - 1]
            dst, ssem, rsem, axis = buf_b.at[d, i], send_sems.at[2], recv_b.at[d, i], "z"
        else:
            src = buf_b.at[d, NZ - 2] if j == 0 else buf_xb.at[d, j - 1]
            dst, ssem, rsem, axis = buf_xb.at[d, j], send_sems.at[3], recv_xb.at[d, j], "x"
        target = wrap(x + sign[d], NX) if axis == "x" else wrap(z + sign[d], NZ)
        return pltpu.make_async_remote_copy(
            src_ref=src, dst_ref=dst, send_sem=ssem, recv_sem=rsem,
            device_id={axis: target}, device_id_type=MESH,
        )

    def add_own(task):
        kind, d, j, s = task
        if kind == "A":
            i = j * (NX - 1) + s
            buf_a[d, i] = buf_a[d, i] + own_a(d, j, s + 1)[...]
        elif kind == "ZA":
            mine = buf_a[d, (s + 1) * (NX - 1) + NX - 2]
            if s == NZ - 2:
                grad[d, :RA] = buf_za[d, s] + mine
            else:
                buf_za[d, s] = buf_za[d, s] + mine
        elif kind == "B":
            i = j * (NZ - 1) + s
            buf_b[d, i] = buf_b[d, i] + own_b(d, j, s + 1)[...]
        else:
            mine = buf_b[d, (j + 1) * (NZ - 1) + NZ - 2]
            if j == NX - 2:
                grad[d, RA:] = buf_xb[d, j] + mine
            else:
                buf_xb[d, j] = buf_xb[d, j] + mine

    def product(d, s, h, start):
        out = jnp.dot(cot_t[...], act[d, h], preferred_element_type=F32)
        for t in range(TILES // 2):
            rows = pl.ds(start + t * ROWS, ROWS)
            for q in range(NZ):
                part[d, s, q, rows] = out[q * ROWS : (q + 1) * ROWS, t * 128 : (t + 1) * 128]

    half_rows = BLOCK_ROWS // 2

    def matmul(d, s, h):
        if s == 0:
            loads[("act", d, h)].wait()
        if h:
            loads[("cot", d, s)].wait()
            cot_t[...] = jnp.transpose(cot[d, s])
        if h != 1:
            load_next()
        if h == 2:

            @pl.loop(0, 2)
            def _(n):
                product(d, s, n, pl.multiple_of(n * half_rows, half_rows))
        else:
            product(d, s, h, h * half_rows)

    def old_state():
        for name in ("mcode", "scode", "mscale", "sscale"):
            loads[name].wait()
        for d in range(LAYERS):
            moment_scale = own_block(mscale[d], y)
            square_scale = own_block(sscale[d], y)
            for t in range(TILES):
                rows, cols = pl.ds(t * ROWS, ROWS), pl.ds(t * 128, 128)
                old_m[d, rows] = beta_one * (mcode[d, :, cols].astype(F32) * moment_scale)
                old_s[d, rows] = beta_two * (scode[d, :, cols].astype(F32) * square_scale)

    first = True
    for task, sends in task_order():
        if task[0] == "M":
            matmul(task[1], task[2], task[3])
            if first:
                pl.semaphore_wait(barrier, len(peers))
                first = False
        else:
            copy_of(task).wait_recv()
            add_own(task)
        for send in sends:
            copy_of(send).start()
        if task == ("M", 1, NX - 1, 2):
            old_state()

    grad_copies = [pltpu.make_async_copy(grad.at[d], grad_out.at[d], out_sems.at[d]) for d in range(LAYERS)]
    for copy in grad_copies:
        copy.start()

    lanes = [jnp.zeros((8, 128), F32) for _ in range(8)]
    for d in range(LAYERS):
        for i in range(BLOCK_ROWS // 8):
            v = grad[d, i * 8 : (i + 1) * 8, :]
            lanes[i % 8] = lanes[i % 8] + v * v
    while len(lanes) > 1:
        lanes = [p + q for p, q in zip(lanes[::2], lanes[1::2])]
    line = jnp.sum(lanes[0], axis=0, keepdims=True)
    def all_of(ref, k):
        return pltpu.make_async_remote_copy(
            src_ref=ref, dst_ref=ref, send_sem=send_sems.at[k], recv_sem=recv_sems.at[max(k - 4, 0)],
            device_id={"core": 1 - c}, device_id_type=MESH,
        )

    base = 0
    for n, stage in enumerate(stages):
        norm_send[n] = line
        for i, peer in enumerate(stage):
            pltpu.make_async_remote_copy(
                src_ref=norm_send.at[n], dst_ref=norm_recv.at[base + i],
                send_sem=send_sems.at[4 + n], recv_sem=recv_sems.at[n],
                device_id=peer, device_id_type=MESH,
            ).start()
        if n == 0:
            for k, buf in enumerate((buf_a, buf_za, buf_b, buf_xb)):
                all_of(buf, k).wait_send()
        incoming = all_of(norm_recv.at[pl.ds(base, len(stage))], 4 + n)
        incoming.wait_recv()
        sums = [norm_recv[base + i] for i in range(len(stage))]
        while len(sums) > 1:
            sums = [sum(sums[i : i + 2]) for i in range(0, len(sums), 2)]
        line = line + sums[0]
        base += len(stage)
    total_sq = jnp.sum(line, axis=1, keepdims=True)
    rms = jnp.sqrt(total_sq / float(LAYERS * KV * D) + norm_eps)
    clip = jnp.minimum(1.0, 1.0 / rms)

    rows = []
    for d in range(LAYERS):
        top_moment = jnp.zeros((ROWS, 128), F32)
        top_square = jnp.zeros((ROWS, 128), F32)
        for t in range(TILES):
            moment, square = moments(
                clip, grad[d, t * ROWS : (t + 1) * ROWS, :],
                old_m[d, t * ROWS : (t + 1) * ROWS, :], old_s[d, t * ROWS : (t + 1) * ROWS, :],
            )
            top_moment = jnp.maximum(top_moment, jnp.abs(moment))
            top_square = jnp.maximum(top_square, square)
        rows.append(to_row(jnp.max(top_moment, axis=1, keepdims=True)))
        rows.append(to_row(jnp.max(top_square, axis=1, keepdims=True)))
    top = jnp.concatenate(rows + [jnp.zeros((4, 128), F32)], axis=0)

    own_top[...] = top
    for i, ((dy, dc), peer) in enumerate(zip(col_steps, col_peers)):
        pltpu.make_async_remote_copy(
            src_ref=own_top, dst_ref=tops.at[i], send_sem=send_sems.at[6], recv_sem=recv_sems.at[2],
            device_id=peer, device_id_type=MESH,
        ).start()
    for n, stage in enumerate(stages):
        all_of(norm_recv.at[pl.ds(0, len(stage))], 4 + n).wait_send()
    for copy in grad_copies:
        copy.wait()
    incoming = all_of(tops, 6)
    incoming.wait_recv()
    same_chip = [i for i, (dy, dc) in enumerate(col_steps) if dy == 0]
    small_out[y] = jnp.maximum(top, tops[same_chip[0]])
    for dy in range(1, NY):
        pair = [tops[i] for i, step in enumerate(col_steps) if step[0] == dy]
        small_out[wrap(y - dy, NY)] = jnp.maximum(*pair)
    small_out[NY] = jnp.broadcast_to(clip, (8, 128))
    small_copy = pltpu.make_async_copy(small_out, small_hbm, out_sems.at[LAYERS])
    small_copy.start()
    incoming.wait_send()
    small_copy.wait()


def to_row(column):
    diagonal = lax.broadcasted_iota(jnp.int32, (ROWS, 128), 0) == lax.broadcasted_iota(
        jnp.int32, (ROWS, 128), 1
    )
    return jnp.sum(jnp.where(diagonal, column, 0.0), axis=0, keepdims=True)


def to_column(row):
    diagonal = lax.broadcasted_iota(jnp.int32, (ROWS, ROWS), 0) == lax.broadcasted_iota(
        jnp.int32, (ROWS, ROWS), 1
    )
    return jnp.sum(jnp.where(diagonal, row, 0.0), axis=1, keepdims=True)


def own_block(scales, block):
    mine = lax.broadcasted_iota(jnp.int32, (NY, ROWS), 0) == block
    return to_column(jnp.sum(jnp.where(mine, scales, 0.0), axis=0, keepdims=True))


def moments(clip, grad, old_moment, old_square):
    grad_now = clip * grad
    moment = old_moment + (1.0 - beta_one) * grad_now
    square = old_square + (1.0 - beta_two) * grad_now * grad_now
    return moment, square


def update_kernel(
    grad, small, master, mcode, scode, mscale, sscale,
    weights_out, mcode_out, scode_out, mscale_out, sscale_out,
):
    d = pl.program_id(0)
    y = lax.axis_index("y")
    clip = small[NY, :1, :1]
    correct_one = 1.0 - beta_one**STEP
    correct_two = 1.0 - beta_two**STEP
    moment_scale = own_block(mscale[d], y)
    square_scale = own_block(sscale[d], y)
    moment_div = to_column(small[y, pl.ds(2 * d, 1), :ROWS]) + scale_eps
    square_div = to_column(small[y, pl.ds(2 * d + 1, 1), :ROWS]) + scale_eps
    for t in range(TILES):
        cols = pl.ds(t * 128, 128)
        moment, square = moments(
            clip, grad[d, t * ROWS : (t + 1) * ROWS, :],
            beta_one * (mcode[d, :, cols].astype(F32) * moment_scale),
            beta_two * (scode[d, :, cols].astype(F32) * square_scale),
        )
        mcode_out[0, :, cols] = (moment / moment_div).astype(jnp.bfloat16)
        scode_out[0, :, cols] = (square / square_div).astype(jnp.bfloat16)
        ratio = moment / correct_one / (jnp.sqrt(square / correct_two) + adam_eps)
        weights = master[d, :, cols]
        weights_out[0, :, cols] = weights - learn_rate * (decay_rate * weights + ratio)
    for b in range(NY):
        mscale_out[0, b : b + 1, :] = small[b, pl.ds(2 * d, 1), :ROWS]
        sscale_out[0, b : b + 1, :] = small[b, pl.ds(2 * d + 1, 1), :ROWS]


def local(
    activations, cotangent, master_weights, moment_codes, square_codes, moment_scales, square_scales
):
    shard = (LAYERS, ROWS, COLS)
    scales = (LAYERS, NY, ROWS)
    any_spec = pl.BlockSpec(memory_space=pl.ANY)
    vmem_spec = pl.BlockSpec(memory_space=pltpu.VMEM)
    sems = pltpu.SemaphoreType.DMA
    n_norm = NX * NY - 1 + NZ * NC - 1
    block = (LAYERS, BLOCK_ROWS, 128)
    scales_in = (jnp.transpose(moment_scales, (0, 2, 1)), jnp.transpose(square_scales, (0, 2, 1)))
    grad, small = pl.pallas_call(
        kernel,
        out_shape=(
            jax.ShapeDtypeStruct(block, F32),
            jax.ShapeDtypeStruct((NY + 1, 8, 128), F32),
        ),
        in_specs=[pl.BlockSpec(memory_space=pltpu.HBM)] * 6,
        out_specs=[any_spec, any_spec],
        scratch_shapes=[
            pltpu.VMEM((LAYERS, 2, TOK, COLS // 2), jnp.bfloat16),
            pltpu.VMEM((LAYERS, NX, TOK, XROWS), jnp.bfloat16),
            pltpu.VMEM((XROWS, TOK), jnp.bfloat16),
            pltpu.VMEM(shard, jnp.bfloat16),
            pltpu.VMEM(shard, jnp.bfloat16),
            pltpu.VMEM(scales, F32),
            pltpu.VMEM(scales, F32),
            pltpu.VMEM((LAYERS, NX, NZ, BLOCK_ROWS, 128), F32),
            pltpu.VMEM((2, NZ * (NX - 1), RA, 128), F32),
            pltpu.VMEM((2, NZ - 1, RA, 128), F32),
            pltpu.VMEM((2, NX * (NZ - 1), RB, 128), F32),
            pltpu.VMEM((2, NX - 1, RB, 128), F32),
            pltpu.VMEM(block, F32),
            pltpu.VMEM(block, F32),
            pltpu.VMEM(block, F32),
            pltpu.VMEM((2, 1, 128), F32),
            pltpu.VMEM((n_norm, 1, 128), F32),
            pltpu.VMEM((8, 128), F32),
            pltpu.VMEM((NY * NC - 1, 8, 128), F32),
            pltpu.VMEM((NY + 1, 8, 128), F32),
            sems((2 * (NX + 2) + 4,)), sems((7,)), sems((3,)),
            sems((2, 4, NX - 1)), sems((2, NZ - 1)), sems((2, NX * (NZ - 1))), sems((2, NX - 1)),
            sems((LAYERS + 1,)),
        ],
        compiler_params=pltpu.CompilerParams(
            collective_id=0, has_side_effects=True, vmem_limit_bytes=51 * 1024 * 1024
        ),
    )(*(
        pltpu.with_memory_space_constraint(a, pltpu.HBM)
        for a in (activations, cotangent, moment_codes, square_codes, *scales_in)
    ))
    outs = pl.pallas_call(
        update_kernel,
        out_shape=(
            jax.ShapeDtypeStruct(shard, F32),
            jax.ShapeDtypeStruct(shard, jnp.bfloat16),
            jax.ShapeDtypeStruct(shard, jnp.bfloat16),
            jax.ShapeDtypeStruct(scales, F32),
            jax.ShapeDtypeStruct(scales, F32),
        ),
        grid=(LAYERS,),
        in_specs=[vmem_spec] * 7,
        out_specs=[pl.BlockSpec((1, ROWS, COLS), lambda d: (d, 0, 0))] * 3
        + [pl.BlockSpec((1, NY, ROWS), lambda d: (d, 0, 0))] * 2,
        compiler_params=pltpu.CompilerParams(vmem_limit_bytes=8 * 1024 * 1024),
    )(grad, small, master_weights, moment_codes, square_codes, *scales_in)
    return (*outs[:3], jnp.transpose(outs[3], (0, 2, 1)), jnp.transpose(outs[4], (0, 2, 1)))


def solution(mesh):
    split = Mesh(mesh.devices.reshape(NX, NZ, NY, NC), ("x", "z", "y", "core"))
    dp, col = ("x", "z"), ("y", "core")
    big, scale = P(None, dp, col), P(None, dp, None)
    return jax.shard_map(
        local,
        mesh=split,
        in_specs=(big, scale, big, big, big, scale, scale),
        out_specs=(big, big, big, scale, scale),
        check_vma=False,
    )
```

```python
import functools
import heapq

import jax
import jax.numpy as jnp
from jax import lax
from jax.experimental import pallas as pl
from jax.experimental.pallas import tpu as pltpu
from jax.sharding import Mesh
from jax.sharding import PartitionSpec as P

D = 8192
KV = 2048
BLOCK = 2048
LAYERS = 2
STEP = 10

beta_one = 0.9
beta_two = 0.999
learn_rate = 0.001
decay_rate = 0.1
adam_eps = 1e-08
scale_eps = 1e-06
norm_eps = 1e-06

NX, NZ, NY, NC = 4, 8, 4, 2
ROWS = KV // (NX * NZ)
COLS = D // (NY * NC)
TOK = 896
XROWS = ROWS * NZ
TILES = COLS // 128
BLOCK_ROWS = TILES * ROWS
RA = 304
RB = BLOCK_ROWS - RA
WINDOW_A, WINDOW_B = 2, 4
MESH = pl.DeviceIdType.MESH
F32 = jnp.float32


def task_order(rate=44e3, latency=2.5, add=0.2, matmul=2.0):
    bytes_a, bytes_b = RA * 512, RB * 512
    now, order, free, heap, seen = 0.0, [], {}, [], set()
    matmuls = [("M", d, 0, h) for d in (0, 1) for h in (1, 0)]
    matmuls += [("M", d, s, 2) for s in range(1, NX) for d in (0, 1)]
    arrived, count, serial = [], 0, 0
    total = 2 * (NZ * (NX - 1) + NZ - 1 + NX * (NZ - 1) + NX - 1)

    def ready(task):
        kind, d, j, s = task
        need = {
            "A": ("M", d, s + 1, 2),
            "B": ("M", d, j, 2 if j else 1),
            "ZA": ("A", d, s + 1, NX - 2),
            "XB": ("B", d, j + 1, NZ - 2),
        }[kind]
        return need in seen

    def enabled(task):
        kind, d, j, s = task
        out = []
        if kind == "M":
            if s == 0:
                out += [("A", d, q, 0) for q in range(WINDOW_A)]
            elif j < WINDOW_B:
                out.append(("B", d, j, 0))
        elif kind == "A":
            if s < NX - 2:
                out.append(("A", d, j, s + 1))
            else:
                if j == 0:
                    out.append(("ZA", d, 0, 0))
                if j + WINDOW_A < NZ:
                    out.append(("A", d, j + WINDOW_A, 0))
        elif kind == "B":
            if s < NZ - 2:
                out.append(("B", d, j, s + 1))
            else:
                if j == 0:
                    out.append(("XB", d, 0, 0))
                if j + WINDOW_B < NX:
                    out.append(("B", d, j + WINDOW_B, 0))
        elif kind == "ZA":
            if s < NZ - 2:
                out.append(("ZA", d, 0, s + 1))
        elif kind == "XB":
            if j < NX - 2:
                out.append(("XB", d, j + 1, 0))
        return out

    while count < total or matmuls:
        while heap and heap[0][0] <= now:
            arrived.append(heapq.heappop(heap))
        able = [a for a in arrived if ready(a[2])]
        if able:
            first = min(able)
            arrived.remove(first)
            task = first[2]
            now += add
            count += 1
        elif matmuls:
            task = matmuls.pop(0)
            now += matmul if task[3] == 2 else matmul / 2
        else:
            now = max(now, heap[0][0])
            continue
        seen.add(task)
        sends = enabled(task)
        for send in sends:
            link = ("x" if send[0] in ("A", "XB") else "z", send[1])
            size = bytes_a if send[0] in ("A", "ZA") else bytes_b
            free[link] = max(now, free.get(link, 0.0)) + size / rate
            heapq.heappush(heap, (free[link] + latency, serial, send))
            serial += 1
        order.append((task, sends))
    return order


def kernel(
    act_hbm, cot_hbm, mcode_hbm, scode_hbm, mscale_hbm, sscale_hbm,
    grad_out, small_out,
    act, cot, cot_t, mcode, scode, mscale, sscale,
    part, buf_a, buf_za, buf_b, buf_xb, grad, old_m, old_s, norm_send, norm_recv, own_top,
    in_sems, send_sems, recv_sems, recv_a, recv_za, recv_b, recv_xb, out_sems,
):
    x, z, y, c = (lax.axis_index(n) for n in ("x", "z", "y", "core"))
    sign = (1, -1)

    def wrap(v, n):
        return lax.rem(v + 2 * n, n)

    def xrel(d, s):
        return wrap(x - sign[d] * (1 + s), NX)

    def zrel(d, s):
        return wrap(z - sign[d] * (1 + s), NZ)

    loads = {}

    def load(name, src, dst, k):
        loads[name] = pltpu.make_async_copy(src, dst, in_sems.at[k])
        loads[name].start()

    def cot_columns(d, s):
        return pl.ds(pl.multiple_of(xrel(d, s) * XROWS, XROWS), XROWS)

    half = COLS // 2

    def cot_load(d, s):
        return (("cot", d, s), cot_hbm.at[d, :, cot_columns(d, s)], cot.at[d, s])

    def act_load(d, h):
        return (("act", d, h), act_hbm.at[d, :, pl.ds(h * half, half)], act.at[d, h])

    groups = [[cot_load(d, 0), act_load(d, 1), act_load(d, 0)] for d in (0, 1)]
    groups += [[cot_load(d, s)] for s in range(1, NX) for d in (0, 1)]
    groups.append([
        ("mcode", mcode_hbm, mcode), ("scode", scode_hbm, scode),
        ("mscale", mscale_hbm, mscale), ("sscale", sscale_hbm, sscale),
    ])

    def load_next():
        if groups:
            for name, src, dst in groups.pop(0):
                load(name, src, dst, len(loads))

    load_next()

    col_steps = [(i, j) for i in range(NY) for j in range(NC) if i or j]
    barrier = pltpu.get_barrier_semaphore()
    col_peers = [{"y": wrap(y + i, NY), "core": wrap(c + j, NC)} for i, j in col_steps]
    stages = (
        [{"x": wrap(x + i, NX), "y": wrap(y + j, NY)} for i in range(NX) for j in range(NY) if i or j],
        [{"z": wrap(z + i, NZ), "core": wrap(c + j, NC)} for i in range(NZ) for j in range(NC) if i or j],
    )
    peers = [{"x": wrap(x + i, NX)} for i in sign] + [{"z": wrap(z + i, NZ)} for i in sign] + col_peers
    for peer in peers:
        pl.semaphore_signal(barrier, inc=1, device_id=peer, device_id_type=MESH)

    def own_a(d, j, s):
        return part.at[d, s, zrel(d, j), pl.ds(0, RA)]

    def own_b(d, j, s):
        return part.at[d, j, zrel(d, s), pl.ds(RA, RB)]

    def copy_of(task):
        kind, d, j, s = task
        if kind == "A":
            i = j * (NX - 1) + s
            src = own_a(d, j, 0) if s == 0 else buf_a.at[d, i - 1]
            dst, ssem, rsem, axis = buf_a.at[d, i], send_sems.at[0], recv_a.at[d, j % 4, s], "x"
        elif kind == "ZA":
            src = buf_a.at[d, NX - 2] if s == 0 else buf_za.at[d, s - 1]
            dst, ssem, rsem, axis = buf_za.at[d, s], send_sems.at[1], recv_za.at[d, s], "z"
        elif kind == "B":
            i = j * (NZ - 1) + s
            src = own_b(d, j, 0) if s == 0 else buf_b.at[d, i - 1]
            dst, ssem, rsem, axis = buf_b.at[d, i], send_sems.at[2], recv_b.at[d, i], "z"
        else:
            src = buf_b.at[d, NZ - 2] if j == 0 else buf_xb.at[d, j - 1]
            dst, ssem, rsem, axis = buf_xb.at[d, j], send_sems.at[3], recv_xb.at[d, j], "x"
        target = wrap(x + sign[d], NX) if axis == "x" else wrap(z + sign[d], NZ)
        return pltpu.make_async_remote_copy(
            src_ref=src, dst_ref=dst, send_sem=ssem, recv_sem=rsem,
            device_id={axis: target}, device_id_type=MESH,
        )

    squares = [jnp.zeros((8, 128), F32) for _ in range(4)]

    def finish(d, row, value):
        grad[d, row : row + value.shape[0]] = value
        for i in range(value.shape[0] // 8):
            v = value[i * 8 : (i + 1) * 8, :]
            squares[i % 4] = squares[i % 4] + v * v

    def add_own(task):
        kind, d, j, s = task
        if kind == "A":
            i = j * (NX - 1) + s
            buf_a[d, i] = buf_a[d, i] + own_a(d, j, s + 1)[...]
        elif kind == "ZA":
            mine = buf_a[d, (s + 1) * (NX - 1) + NX - 2]
            if s == NZ - 2:
                finish(d, 0, buf_za[d, s] + mine)
            else:
                buf_za[d, s] = buf_za[d, s] + mine
        elif kind == "B":
            i = j * (NZ - 1) + s
            buf_b[d, i] = buf_b[d, i] + own_b(d, j, s + 1)[...]
        else:
            mine = buf_b[d, (j + 1) * (NZ - 1) + NZ - 2]
            if j == NX - 2:
                finish(d, RA, buf_xb[d, j] + mine)
            else:
                buf_xb[d, j] = buf_xb[d, j] + mine

    def product(d, s, h, start):
        out = jnp.dot(cot_t[d], act[d, h], preferred_element_type=F32)
        for t in range(TILES // 2):
            rows = pl.ds(start + t * ROWS, ROWS)
            for q in range(NZ):
                part[d, s, q, rows] = out[q * ROWS : (q + 1) * ROWS, t * 128 : (t + 1) * 128]

    half_rows = BLOCK_ROWS // 2

    def matmul(d, s, h):
        if s == 0:
            loads[("act", d, h)].wait()
        if h:
            loads[("cot", d, s)].wait()
        load_next()
        if h:
            cot_t[d] = jnp.transpose(cot[d, s])
        if h == 2:

            @pl.loop(0, 2)
            def _(n):
                product(d, s, n, pl.multiple_of(n * half_rows, half_rows))
        else:
            product(d, s, h, h * half_rows)

    def old_state():
        for name in ("mcode", "scode", "mscale", "sscale"):
            loads[name].wait()
        for d in range(LAYERS):
            moment_scale = own_block(mscale[d], y)
            square_scale = own_block(sscale[d], y)
            for t in range(TILES):
                rows, cols = pl.ds(t * ROWS, ROWS), pl.ds(t * 128, 128)
                old_m[d, rows] = beta_one * (mcode[d, :, cols].astype(F32) * moment_scale)
                old_s[d, rows] = beta_two * (scode[d, :, cols].astype(F32) * square_scale)

    first = True
    for task, sends in task_order():
        if task[0] == "M":
            matmul(task[1], task[2], task[3])
            if first:
                pl.semaphore_wait(barrier, len(peers))
                first = False
        else:
            copy_of(task).wait_recv()
            add_own(task)
        for send in sends:
            copy_of(send).start()
        if task == ("M", 1, NX - 1, 2):
            old_state()

    grad_copies = [pltpu.make_async_copy(grad.at[d], grad_out.at[d], out_sems.at[d]) for d in range(LAYERS)]
    for copy in grad_copies:
        copy.start()

    lanes = squares
    while len(lanes) > 1:
        lanes = [p + q for p, q in zip(lanes[::2], lanes[1::2])]
    line = jnp.sum(lanes[0], axis=0, keepdims=True)
    def all_of(ref, k):
        return pltpu.make_async_remote_copy(
            src_ref=ref, dst_ref=ref, send_sem=send_sems.at[k], recv_sem=recv_sems.at[max(k - 4, 0)],
            device_id={"core": 1 - c}, device_id_type=MESH,
        )

    base = 0
    for n, stage in enumerate(stages):
        norm_send[n] = line
        for i, peer in enumerate(stage):
            pltpu.make_async_remote_copy(
                src_ref=norm_send.at[n], dst_ref=norm_recv.at[base + i],
                send_sem=send_sems.at[4 + n], recv_sem=recv_sems.at[n],
                device_id=peer, device_id_type=MESH,
            ).start()
        if n == 0:
            for k, buf in enumerate((buf_a, buf_za, buf_b, buf_xb)):
                all_of(buf, k).wait_send()
        incoming = all_of(norm_recv.at[pl.ds(base, len(stage))], 4 + n)
        incoming.wait_recv()
        sums = [norm_recv[base + i] for i in range(len(stage))]
        while len(sums) > 1:
            sums = [sum(sums[i : i + 2]) for i in range(0, len(sums), 2)]
        line = line + sums[0]
        base += len(stage)
    total_sq = jnp.sum(line, axis=1, keepdims=True)
    rms = jnp.sqrt(total_sq / float(LAYERS * KV * D) + norm_eps)
    clip = jnp.minimum(1.0, 1.0 / rms)

    rows = []
    for d in range(LAYERS):
        top_moment = jnp.zeros((ROWS, 128), F32)
        top_square = jnp.zeros((ROWS, 128), F32)
        for t in range(TILES):
            moment, square = moments(
                clip, grad[d, t * ROWS : (t + 1) * ROWS, :],
                old_m[d, t * ROWS : (t + 1) * ROWS, :], old_s[d, t * ROWS : (t + 1) * ROWS, :],
            )
            top_moment = jnp.maximum(top_moment, jnp.abs(moment))
            top_square = jnp.maximum(top_square, square)
        rows.append(to_row(jnp.max(top_moment, axis=1, keepdims=True)))
        rows.append(to_row(jnp.max(top_square, axis=1, keepdims=True)))
    own_top[0] = jnp.concatenate(rows + [jnp.zeros((4, 128), F32)], axis=0)
    own_top[1] = jnp.broadcast_to(clip, (8, 128))
    for peer in col_peers:
        pltpu.make_async_remote_copy(
            src_ref=own_top.at[0], dst_ref=small_out.at[y * NC + c],
            send_sem=send_sems.at[6], recv_sem=recv_sems.at[2],
            device_id=peer, device_id_type=MESH,
        ).start()
    own_copies = [
        pltpu.make_async_copy(own_top.at[0], small_out.at[y * NC + c], out_sems.at[LAYERS]),
        pltpu.make_async_copy(own_top.at[1], small_out.at[NY * NC], out_sems.at[LAYERS + 1]),
    ]
    for copy in own_copies:
        copy.start()
    for n, stage in enumerate(stages):
        all_of(norm_recv.at[pl.ds(0, len(stage))], 4 + n).wait_send()
    for copy in grad_copies + own_copies:
        copy.wait()
    incoming = all_of(small_out.at[pl.ds(0, NY * NC - 1)], 6)
    incoming.wait_send()
    incoming.wait_recv()


def to_row(column):
    diagonal = lax.broadcasted_iota(jnp.int32, (ROWS, 128), 0) == lax.broadcasted_iota(
        jnp.int32, (ROWS, 128), 1
    )
    return jnp.sum(jnp.where(diagonal, column, 0.0), axis=0, keepdims=True)


def to_column(row):
    diagonal = lax.broadcasted_iota(jnp.int32, (ROWS, ROWS), 0) == lax.broadcasted_iota(
        jnp.int32, (ROWS, ROWS), 1
    )
    return jnp.sum(jnp.where(diagonal, row, 0.0), axis=1, keepdims=True)


def own_block(scales, block):
    mine = lax.broadcasted_iota(jnp.int32, (NY, ROWS), 0) == block
    return to_column(jnp.sum(jnp.where(mine, scales, 0.0), axis=0, keepdims=True))


def moments(clip, grad, old_moment, old_square):
    grad_now = clip * grad
    moment = old_moment + (1.0 - beta_one) * grad_now
    square = old_square + (1.0 - beta_two) * grad_now * grad_now
    return moment, square


def update_kernel(
    grad, small, master, mcode, scode, mscale, sscale,
    weights_out, mcode_out, scode_out, mscale_out, sscale_out,
):
    d = pl.program_id(0)
    y = lax.axis_index("y")
    clip = small[NY * NC, :1, :1]

    def top(b, kind):
        row = pl.ds(2 * d + kind, 1)
        return jnp.maximum(small[b * NC, row, :ROWS], small[b * NC + 1, row, :ROWS])

    correct_one = 1.0 - beta_one**STEP
    correct_two = 1.0 - beta_two**STEP
    moment_scale = own_block(mscale[d], y)
    square_scale = own_block(sscale[d], y)
    moment_div = to_column(top(y, 0)) + scale_eps
    square_div = to_column(top(y, 1)) + scale_eps
    for t in range(TILES):
        cols = pl.ds(t * 128, 128)
        moment, square = moments(
            clip, grad[d, t * ROWS : (t + 1) * ROWS, :],
            beta_one * (mcode[d, :, cols].astype(F32) * moment_scale),
            beta_two * (scode[d, :, cols].astype(F32) * square_scale),
        )
        mcode_out[0, :, cols] = (moment / moment_div).astype(jnp.bfloat16)
        scode_out[0, :, cols] = (square / square_div).astype(jnp.bfloat16)
        ratio = moment / correct_one / (jnp.sqrt(square / correct_two) + adam_eps)
        weights = master[d, :, cols]
        weights_out[0, :, cols] = weights - learn_rate * (decay_rate * weights + ratio)
    for b in range(NY):
        mscale_out[0, b : b + 1, :] = top(b, 0)
        sscale_out[0, b : b + 1, :] = top(b, 1)


def local(
    activations, cotangent, master_weights, moment_codes, square_codes, moment_scales, square_scales
):
    shard = (LAYERS, ROWS, COLS)
    scales = (LAYERS, NY, ROWS)
    any_spec = pl.BlockSpec(memory_space=pl.ANY)
    vmem_spec = pl.BlockSpec(memory_space=pltpu.VMEM)
    sems = pltpu.SemaphoreType.DMA
    n_norm = NX * NY - 1 + NZ * NC - 1
    block = (LAYERS, BLOCK_ROWS, 128)
    scales_in = (jnp.transpose(moment_scales, (0, 2, 1)), jnp.transpose(square_scales, (0, 2, 1)))
    grad, small = pl.pallas_call(
        kernel,
        out_shape=(
            jax.ShapeDtypeStruct(block, F32),
            jax.ShapeDtypeStruct((NY * NC + 1, 8, 128), F32),
        ),
        in_specs=[pl.BlockSpec(memory_space=pltpu.HBM)] * 6,
        out_specs=[any_spec, any_spec],
        scratch_shapes=[
            pltpu.VMEM((LAYERS, 2, TOK, COLS // 2), jnp.bfloat16),
            pltpu.VMEM((LAYERS, NX, TOK, XROWS), jnp.bfloat16),
            pltpu.VMEM((LAYERS, XROWS, TOK), jnp.bfloat16),
            pltpu.VMEM(shard, jnp.bfloat16),
            pltpu.VMEM(shard, jnp.bfloat16),
            pltpu.VMEM(scales, F32),
            pltpu.VMEM(scales, F32),
            pltpu.VMEM((LAYERS, NX, NZ, BLOCK_ROWS, 128), F32),
            pltpu.VMEM((2, NZ * (NX - 1), RA, 128), F32),
            pltpu.VMEM((2, NZ - 1, RA, 128), F32),
            pltpu.VMEM((2, NX * (NZ - 1), RB, 128), F32),
            pltpu.VMEM((2, NX - 1, RB, 128), F32),
            pltpu.VMEM(block, F32),
            pltpu.VMEM(block, F32),
            pltpu.VMEM(block, F32),
            pltpu.VMEM((2, 1, 128), F32),
            pltpu.VMEM((n_norm, 1, 128), F32),
            pltpu.VMEM((2, 8, 128), F32),
            sems((2 * (NX + 2) + 4,)), sems((7,)), sems((3,)),
            sems((2, 4, NX - 1)), sems((2, NZ - 1)), sems((2, NX * (NZ - 1))), sems((2, NX - 1)),
            sems((LAYERS + 2,)),
        ],
        compiler_params=pltpu.CompilerParams(
            collective_id=0, has_side_effects=True, vmem_limit_bytes=51 * 1024 * 1024
        ),
    )(*(
        pltpu.with_memory_space_constraint(a, pltpu.HBM)
        for a in (activations, cotangent, moment_codes, square_codes, *scales_in)
    ))
    outs = pl.pallas_call(
        update_kernel,
        out_shape=(
            jax.ShapeDtypeStruct(shard, F32),
            jax.ShapeDtypeStruct(shard, jnp.bfloat16),
            jax.ShapeDtypeStruct(shard, jnp.bfloat16),
            jax.ShapeDtypeStruct(scales, F32),
            jax.ShapeDtypeStruct(scales, F32),
        ),
        grid=(LAYERS,),
        in_specs=[vmem_spec] * 7,
        out_specs=[pl.BlockSpec((1, ROWS, COLS), lambda d: (d, 0, 0))] * 3
        + [pl.BlockSpec((1, NY, ROWS), lambda d: (d, 0, 0))] * 2,
        compiler_params=pltpu.CompilerParams(vmem_limit_bytes=8 * 1024 * 1024),
    )(grad, small, master_weights, moment_codes, square_codes, *scales_in)
    return (*outs[:3], jnp.transpose(outs[3], (0, 2, 1)), jnp.transpose(outs[4], (0, 2, 1)))


def solution(mesh):
    split = Mesh(mesh.devices.reshape(NX, NZ, NY, NC), ("x", "z", "y", "core"))
    dp, col = ("x", "z"), ("y", "core")
    big, scale = P(None, dp, col), P(None, dp, None)
    return jax.shard_map(
        local,
        mesh=split,
        in_specs=(big, scale, big, big, big, scale, scale),
        out_specs=(big, big, big, scale, scale),
        check_vma=False,
    )
```

```python
import functools
import heapq

import jax
import jax.numpy as jnp
from jax import lax
from jax.experimental import pallas as pl
from jax.experimental.pallas import tpu as pltpu
from jax.sharding import Mesh
from jax.sharding import PartitionSpec as P

D = 8192
KV = 2048
BLOCK = 2048
LAYERS = 2
STEP = 10

beta_one = 0.9
beta_two = 0.999
learn_rate = 0.001
decay_rate = 0.1
adam_eps = 1e-08
scale_eps = 1e-06
norm_eps = 1e-06

NX, NZ, NY, NC = 4, 8, 4, 2
ROWS = KV // (NX * NZ)
COLS = D // (NY * NC)
TOK = 896
XROWS = ROWS * NZ
TILES = COLS // 128
BLOCK_ROWS = TILES * ROWS
RA = 304
RB = BLOCK_ROWS - RA
WINDOW_A, WINDOW_B = 2, 4
MESH = pl.DeviceIdType.MESH
F32 = jnp.float32


def task_order(rate=44e3, latency=2.5, add=0.2, matmul=2.0):
    bytes_a, bytes_b = RA * 512, RB * 512
    now, order, free, heap, seen = 0.0, [], {}, [], set()
    matmuls = [("M", d, 0, h) for d in (0, 1) for h in (1, 0)]
    matmuls += [("M", d, s, 2) for s in range(1, NX) for d in (0, 1)]
    arrived, count, serial = [], 0, 0
    total = 2 * (NZ * (NX - 1) + NZ - 1 + NX * (NZ - 1) + NX - 1)

    def ready(task):
        kind, d, j, s = task
        need = {
            "A": ("M", d, s + 1, 2),
            "B": ("M", d, j, 2 if j else 1),
            "ZA": ("A", d, s + 1, NX - 2),
            "XB": ("B", d, j + 1, NZ - 2),
        }[kind]
        return need in seen

    def enabled(task):
        kind, d, j, s = task
        out = []
        if kind == "M":
            if s == 0:
                out += [("A", d, q, 0) for q in range(WINDOW_A)]
            elif j < WINDOW_B:
                out.append(("B", d, j, 0))
        elif kind == "A":
            if s < NX - 2:
                out.append(("A", d, j, s + 1))
            else:
                if j == 0:
                    out.append(("ZA", d, 0, 0))
                if j + WINDOW_A < NZ:
                    out.append(("A", d, j + WINDOW_A, 0))
        elif kind == "B":
            if s < NZ - 2:
                out.append(("B", d, j, s + 1))
            else:
                if j == 0:
                    out.append(("XB", d, 0, 0))
                if j + WINDOW_B < NX:
                    out.append(("B", d, j + WINDOW_B, 0))
        elif kind == "ZA":
            if s < NZ - 2:
                out.append(("ZA", d, 0, s + 1))
        elif kind == "XB":
            if j < NX - 2:
                out.append(("XB", d, j + 1, 0))
        return out

    while count < total or matmuls:
        while heap and heap[0][0] <= now:
            arrived.append(heapq.heappop(heap))
        able = [a for a in arrived if ready(a[2])]
        if able:
            first = min(able)
            arrived.remove(first)
            task = first[2]
            now += add
            count += 1
        elif matmuls:
            task = matmuls.pop(0)
            now += matmul if task[3] == 2 else matmul / 2
        else:
            now = max(now, heap[0][0])
            continue
        seen.add(task)
        sends = enabled(task)
        for send in sends:
            link = ("x" if send[0] in ("A", "XB") else "z", send[1])
            size = bytes_a if send[0] in ("A", "ZA") else bytes_b
            free[link] = max(now, free.get(link, 0.0)) + size / rate
            heapq.heappush(heap, (free[link] + latency, serial, send))
            serial += 1
        order.append((task, sends))
    return order


def kernel(
    act_hbm, cot_hbm, mcode_hbm, scode_hbm, mscale_hbm, sscale_hbm,
    grad_out, small_out,
    act, cot, cot_t, mcode, scode, mscale, sscale,
    part, buf_a, buf_za, buf_b, buf_xb, grad, old_m, old_s, norm_send, norm_recv, own_top,
    in_sems, send_sems, recv_sems, recv_a, recv_za, recv_b, recv_xb, out_sems,
):
    x, z, y, c = (lax.axis_index(n) for n in ("x", "z", "y", "core"))
    sign = (1 - 2 * c, 2 * c - 1)

    def wrap(v, n):
        return lax.rem(v + 2 * n, n)

    def xrel(d, s):
        return wrap(x - sign[d] * (1 + s), NX)

    def zrel(d, s):
        return wrap(z - sign[d] * (1 + s), NZ)

    loads = {}

    def load(name, src, dst, k):
        loads[name] = pltpu.make_async_copy(src, dst, in_sems.at[k])
        loads[name].start()

    def cot_columns(d, s):
        return pl.ds(pl.multiple_of(xrel(d, s) * XROWS, XROWS), XROWS)

    half = COLS // 2

    def cot_load(d, s):
        return (("cot", d, s), cot_hbm.at[d, :, cot_columns(d, s)], cot.at[d, s])

    def act_load(d, h):
        return (("act", d, h), act_hbm.at[d, :, pl.ds(h * half, half)], act.at[d, h])

    groups = [[cot_load(d, 0), act_load(d, 1), act_load(d, 0)] for d in (0, 1)]
    groups += [[cot_load(d, s)] for s in range(1, NX) for d in (0, 1)]
    groups.append([
        ("mcode", mcode_hbm, mcode), ("scode", scode_hbm, scode),
        ("mscale", mscale_hbm, mscale), ("sscale", sscale_hbm, sscale),
    ])

    def load_next():
        if groups:
            for name, src, dst in groups.pop(0):
                load(name, src, dst, len(loads))

    load_next()

    col_steps = [(i, j) for i in range(NY) for j in range(NC) if i or j]
    barrier = pltpu.get_barrier_semaphore()
    col_peers = [{"y": wrap(y + i, NY), "core": wrap(c + j, NC)} for i, j in col_steps]
    stages = (
        [{"x": wrap(x + i, NX), "y": wrap(y + j, NY)} for i in range(NX) for j in range(NY) if i or j],
        [{"z": wrap(z + i, NZ), "core": wrap(c + j, NC)} for i in range(NZ) for j in range(NC) if i or j],
    )
    peers = [{"x": wrap(x + i, NX)} for i in (1, -1)] + [{"z": wrap(z + i, NZ)} for i in (1, -1)] + col_peers
    for peer in peers:
        pl.semaphore_signal(barrier, inc=1, device_id=peer, device_id_type=MESH)

    def own_a(d, j, s):
        return part.at[d, s, zrel(d, j), pl.ds(0, RA)]

    def own_b(d, j, s):
        return part.at[d, j, zrel(d, s), pl.ds(RA, RB)]

    def copy_of(task):
        kind, d, j, s = task
        if kind == "A":
            i = j * (NX - 1) + s
            src = own_a(d, j, 0) if s == 0 else buf_a.at[d, i - 1]
            dst, ssem, rsem, axis = buf_a.at[d, i], send_sems.at[0], recv_a.at[d, j % 4, s], "x"
        elif kind == "ZA":
            src = buf_a.at[d, NX - 2] if s == 0 else buf_za.at[d, s - 1]
            dst, ssem, rsem, axis = buf_za.at[d, s], send_sems.at[1], recv_za.at[d, s], "z"
        elif kind == "B":
            i = j * (NZ - 1) + s
            src = own_b(d, j, 0) if s == 0 else buf_b.at[d, i - 1]
            dst, ssem, rsem, axis = buf_b.at[d, i], send_sems.at[2], recv_b.at[d, i], "z"
        else:
            src = buf_b.at[d, NZ - 2] if j == 0 else buf_xb.at[d, j - 1]
            dst, ssem, rsem, axis = buf_xb.at[d, j], send_sems.at[3], recv_xb.at[d, j], "x"
        target = wrap(x + sign[d], NX) if axis == "x" else wrap(z + sign[d], NZ)
        return pltpu.make_async_remote_copy(
            src_ref=src, dst_ref=dst, send_sem=ssem, recv_sem=rsem,
            device_id={axis: target}, device_id_type=MESH,
        )

    squares = [jnp.zeros((8, 128), F32) for _ in range(4)]

    def finish(d, row, value):
        grad[d, row : row + value.shape[0]] = value
        for i in range(value.shape[0] // 8):
            v = value[i * 8 : (i + 1) * 8, :]
            squares[i % 4] = squares[i % 4] + v * v

    def add_own(task):
        kind, d, j, s = task
        if kind == "A":
            i = j * (NX - 1) + s
            buf_a[d, i] = buf_a[d, i] + own_a(d, j, s + 1)[...]
        elif kind == "ZA":
            mine = buf_a[d, (s + 1) * (NX - 1) + NX - 2]
            if s == NZ - 2:
                finish(d, 0, buf_za[d, s] + mine)
            else:
                buf_za[d, s] = buf_za[d, s] + mine
        elif kind == "B":
            i = j * (NZ - 1) + s
            buf_b[d, i] = buf_b[d, i] + own_b(d, j, s + 1)[...]
        else:
            mine = buf_b[d, (j + 1) * (NZ - 1) + NZ - 2]
            if j == NX - 2:
                finish(d, RA, buf_xb[d, j] + mine)
            else:
                buf_xb[d, j] = buf_xb[d, j] + mine

    def product(d, s, h, start):
        out = jnp.dot(cot_t[d], act[d, h], preferred_element_type=F32)
        for t in range(TILES // 2):
            rows = pl.ds(start + t * ROWS, ROWS)
            for q in range(NZ):
                part[d, s, q, rows] = out[q * ROWS : (q + 1) * ROWS, t * 128 : (t + 1) * 128]

    half_rows = BLOCK_ROWS // 2

    def matmul(d, s, h):
        if s == 0:
            loads[("act", d, h)].wait()
        if h:
            loads[("cot", d, s)].wait()
        load_next()
        if h:
            cot_t[d] = jnp.transpose(cot[d, s])
        if h == 2:

            @pl.loop(0, 2)
            def _(n):
                product(d, s, n, pl.multiple_of(n * half_rows, half_rows))
        else:
            product(d, s, h, h * half_rows)

    def old_state():
        for name in ("mcode", "scode", "mscale", "sscale"):
            loads[name].wait()
        for d in range(LAYERS):
            moment_scale = own_block(mscale[d], y)
            square_scale = own_block(sscale[d], y)
            for t in range(TILES):
                rows, cols = pl.ds(t * ROWS, ROWS), pl.ds(t * 128, 128)
                old_m[d, rows] = beta_one * (mcode[d, :, cols].astype(F32) * moment_scale)
                old_s[d, rows] = beta_two * (scode[d, :, cols].astype(F32) * square_scale)

    first = True
    for task, sends in task_order():
        if task[0] == "M":
            matmul(task[1], task[2], task[3])
            if first:
                pl.semaphore_wait(barrier, len(peers))
                first = False
        else:
            copy_of(task).wait_recv()
            add_own(task)
        for send in sends:
            copy_of(send).start()
        if task == ("M", 1, NX - 1, 2):
            old_state()

    grad_copies = [pltpu.make_async_copy(grad.at[d], grad_out.at[d], out_sems.at[d]) for d in range(LAYERS)]
    for copy in grad_copies:
        copy.start()

    lanes = squares
    while len(lanes) > 1:
        lanes = [p + q for p, q in zip(lanes[::2], lanes[1::2])]
    line = jnp.sum(lanes[0], axis=0, keepdims=True)
    def all_of(ref, k):
        return pltpu.make_async_remote_copy(
            src_ref=ref, dst_ref=ref, send_sem=send_sems.at[k], recv_sem=recv_sems.at[max(k - 4, 0)],
            device_id={"core": 1 - c}, device_id_type=MESH,
        )

    base = 0
    for n, stage in enumerate(stages):
        norm_send[n] = line
        for i, peer in enumerate(stage):
            pltpu.make_async_remote_copy(
                src_ref=norm_send.at[n], dst_ref=norm_recv.at[base + i],
                send_sem=send_sems.at[4 + n], recv_sem=recv_sems.at[n],
                device_id=peer, device_id_type=MESH,
            ).start()
        if n == 0:
            for k, buf in enumerate((buf_a, buf_za, buf_b, buf_xb)):
                all_of(buf, k).wait_send()
        incoming = all_of(norm_recv.at[pl.ds(base, len(stage))], 4 + n)
        incoming.wait_recv()
        sums = [norm_recv[base + i] for i in range(len(stage))]
        while len(sums) > 1:
            sums = [sum(sums[i : i + 2]) for i in range(0, len(sums), 2)]
        line = line + sums[0]
        base += len(stage)
    total_sq = jnp.sum(line, axis=1, keepdims=True)
    rms = jnp.sqrt(total_sq / float(LAYERS * KV * D) + norm_eps)
    clip = jnp.minimum(1.0, 1.0 / rms)

    rows = []
    for d in range(LAYERS):
        top_moment = jnp.zeros((ROWS, 128), F32)
        top_square = jnp.zeros((ROWS, 128), F32)
        for t in range(TILES):
            moment, square = moments(
                clip, grad[d, t * ROWS : (t + 1) * ROWS, :],
                old_m[d, t * ROWS : (t + 1) * ROWS, :], old_s[d, t * ROWS : (t + 1) * ROWS, :],
            )
            top_moment = jnp.maximum(top_moment, jnp.abs(moment))
            top_square = jnp.maximum(top_square, square)
        rows.append(to_row(jnp.max(top_moment, axis=1, keepdims=True)))
        rows.append(to_row(jnp.max(top_square, axis=1, keepdims=True)))
    own_top[0] = jnp.concatenate(rows + [jnp.zeros((4, 128), F32)], axis=0)
    own_top[1] = jnp.broadcast_to(clip, (8, 128))
    for peer in col_peers:
        pltpu.make_async_remote_copy(
            src_ref=own_top.at[0], dst_ref=small_out.at[y * NC + c],
            send_sem=send_sems.at[6], recv_sem=recv_sems.at[2],
            device_id=peer, device_id_type=MESH,
        ).start()
    own_copies = [
        pltpu.make_async_copy(own_top.at[0], small_out.at[y * NC + c], out_sems.at[LAYERS]),
        pltpu.make_async_copy(own_top.at[1], small_out.at[NY * NC], out_sems.at[LAYERS + 1]),
    ]
    for copy in own_copies:
        copy.start()
    for n, stage in enumerate(stages):
        all_of(norm_recv.at[pl.ds(0, len(stage))], 4 + n).wait_send()
    for copy in grad_copies + own_copies:
        copy.wait()
    incoming = all_of(small_out.at[pl.ds(0, NY * NC - 1)], 6)
    incoming.wait_send()
    incoming.wait_recv()


def to_row(column):
    diagonal = lax.broadcasted_iota(jnp.int32, (ROWS, 128), 0) == lax.broadcasted_iota(
        jnp.int32, (ROWS, 128), 1
    )
    return jnp.sum(jnp.where(diagonal, column, 0.0), axis=0, keepdims=True)


def to_column(row):
    diagonal = lax.broadcasted_iota(jnp.int32, (ROWS, ROWS), 0) == lax.broadcasted_iota(
        jnp.int32, (ROWS, ROWS), 1
    )
    return jnp.sum(jnp.where(diagonal, row, 0.0), axis=1, keepdims=True)


def own_block(scales, block):
    mine = lax.broadcasted_iota(jnp.int32, (NY, ROWS), 0) == block
    return to_column(jnp.sum(jnp.where(mine, scales, 0.0), axis=0, keepdims=True))


def moments(clip, grad, old_moment, old_square):
    grad_now = clip * grad
    moment = old_moment + (1.0 - beta_one) * grad_now
    square = old_square + (1.0 - beta_two) * grad_now * grad_now
    return moment, square


def update_kernel(
    grad, small, master, mcode, scode, mscale, sscale,
    weights_out, mcode_out, scode_out, mscale_out, sscale_out,
):
    d = pl.program_id(0)
    y = lax.axis_index("y")
    clip = small[NY * NC, :1, :1]

    def top(b, kind):
        row = pl.ds(2 * d + kind, 1)
        return jnp.maximum(small[b * NC, row, :ROWS], small[b * NC + 1, row, :ROWS])

    correct_one = 1.0 - beta_one**STEP
    correct_two = 1.0 - beta_two**STEP
    moment_scale = own_block(mscale[d], y)
    square_scale = own_block(sscale[d], y)
    moment_div = to_column(top(y, 0)) + scale_eps
    square_div = to_column(top(y, 1)) + scale_eps
    for t in range(TILES):
        cols = pl.ds(t * 128, 128)
        moment, square = moments(
            clip, grad[d, t * ROWS : (t + 1) * ROWS, :],
            beta_one * (mcode[d, :, cols].astype(F32) * moment_scale),
            beta_two * (scode[d, :, cols].astype(F32) * square_scale),
        )
        mcode_out[0, :, cols] = (moment / moment_div).astype(jnp.bfloat16)
        scode_out[0, :, cols] = (square / square_div).astype(jnp.bfloat16)
        ratio = moment / correct_one / (jnp.sqrt(square / correct_two) + adam_eps)
        weights = master[d, :, cols]
        weights_out[0, :, cols] = weights - learn_rate * (decay_rate * weights + ratio)
    for b in range(NY):
        mscale_out[0, b : b + 1, :] = top(b, 0)
        sscale_out[0, b : b + 1, :] = top(b, 1)


def local(
    activations, cotangent, master_weights, moment_codes, square_codes, moment_scales, square_scales
):
    shard = (LAYERS, ROWS, COLS)
    scales = (LAYERS, NY, ROWS)
    any_spec = pl.BlockSpec(memory_space=pl.ANY)
    vmem_spec = pl.BlockSpec(memory_space=pltpu.VMEM)
    sems = pltpu.SemaphoreType.DMA
    n_norm = NX * NY - 1 + NZ * NC - 1
    block = (LAYERS, BLOCK_ROWS, 128)
    scales_in = (jnp.transpose(moment_scales, (0, 2, 1)), jnp.transpose(square_scales, (0, 2, 1)))
    grad, small = pl.pallas_call(
        kernel,
        out_shape=(
            jax.ShapeDtypeStruct(block, F32),
            jax.ShapeDtypeStruct((NY * NC + 1, 8, 128), F32),
        ),
        in_specs=[pl.BlockSpec(memory_space=pltpu.HBM)] * 6,
        out_specs=[any_spec, any_spec],
        scratch_shapes=[
            pltpu.VMEM((LAYERS, 2, TOK, COLS // 2), jnp.bfloat16),
            pltpu.VMEM((LAYERS, NX, TOK, XROWS), jnp.bfloat16),
            pltpu.VMEM((LAYERS, XROWS, TOK), jnp.bfloat16),
            pltpu.VMEM(shard, jnp.bfloat16),
            pltpu.VMEM(shard, jnp.bfloat16),
            pltpu.VMEM(scales, F32),
            pltpu.VMEM(scales, F32),
            pltpu.VMEM((LAYERS, NX, NZ, BLOCK_ROWS, 128), F32),
            pltpu.VMEM((2, NZ * (NX - 1), RA, 128), F32),
            pltpu.VMEM((2, NZ - 1, RA, 128), F32),
            pltpu.VMEM((2, NX * (NZ - 1), RB, 128), F32),
            pltpu.VMEM((2, NX - 1, RB, 128), F32),
            pltpu.VMEM(block, F32),
            pltpu.VMEM(block, F32),
            pltpu.VMEM(block, F32),
            pltpu.VMEM((2, 1, 128), F32),
            pltpu.VMEM((n_norm, 1, 128), F32),
            pltpu.VMEM((2, 8, 128), F32),
            sems((2 * (NX + 2) + 4,)), sems((7,)), sems((3,)),
            sems((2, 4, NX - 1)), sems((2, NZ - 1)), sems((2, NX * (NZ - 1))), sems((2, NX - 1)),
            sems((LAYERS + 2,)),
        ],
        compiler_params=pltpu.CompilerParams(
            collective_id=0, has_side_effects=True, vmem_limit_bytes=51 * 1024 * 1024
        ),
    )(*(
        pltpu.with_memory_space_constraint(a, pltpu.HBM)
        for a in (activations, cotangent, moment_codes, square_codes, *scales_in)
    ))
    outs = pl.pallas_call(
        update_kernel,
        out_shape=(
            jax.ShapeDtypeStruct(shard, F32),
            jax.ShapeDtypeStruct(shard, jnp.bfloat16),
            jax.ShapeDtypeStruct(shard, jnp.bfloat16),
            jax.ShapeDtypeStruct(scales, F32),
            jax.ShapeDtypeStruct(scales, F32),
        ),
        grid=(LAYERS,),
        in_specs=[vmem_spec] * 7,
        out_specs=[pl.BlockSpec((1, ROWS, COLS), lambda d: (d, 0, 0))] * 3
        + [pl.BlockSpec((1, NY, ROWS), lambda d: (d, 0, 0))] * 2,
        compiler_params=pltpu.CompilerParams(vmem_limit_bytes=8 * 1024 * 1024),
    )(grad, small, master_weights, moment_codes, square_codes, *scales_in)
    return (*outs[:3], jnp.transpose(outs[3], (0, 2, 1)), jnp.transpose(outs[4], (0, 2, 1)))


def solution(mesh):
    split = Mesh(mesh.devices.reshape(NX, NZ, NY, NC), ("x", "z", "y", "core"))
    dp, col = ("x", "z"), ("y", "core")
    big, scale = P(None, dp, col), P(None, dp, None)
    return jax.shard_map(
        local,
        mesh=split,
        in_specs=(big, scale, big, big, big, scale, scale),
        out_specs=(big, big, big, scale, scale),
        check_vma=False,
    )
```
